32 devices in a mesh: samp: 4 (over z), seq: 8 (over y, x, core).
Axes of the slice: x: 2, y: 2, z: 4, core: 2. Of those that a mesh axis runs over, the one named last changes fastest.
Arguments:
- queries: bfloat16 [4, 4096, 3584], P('samp', 'seq'), may hold values from -200 to 200
- keys: bfloat16 [4, 4096, 512], P('samp', 'seq'), may hold values from -6 to 6
- values: bfloat16 [4, 4096, 512], P('samp', 'seq'), may hold values from -6 to 6
- reg_owner: int32 [4], P('samp'), may hold values from 0 to 7
- block_lists: int32 [4, 32, 8], P('samp', 'seq'), may hold values from 0 to 31, as said below
- list_counts: int32 [4, 32], P('samp', 'seq'), may hold values from 0 to 8, as said below
- image_blocks: int32 [4, 32], P('samp', 'seq'), may hold values from 0 to 1, as said below
Outputs:
- attended: bfloat16 [4, 4096, 3584], P('samp', 'seq')
The draws below stay inside these ranges and needn't reach their ends.
Inputs may be any that keep to these rules, and one draw needn't show every extreme that they name: `block_lists`: block b lies on sequence index b // 4. Entry t of a list is used only where t < the block's count, unused entries are 0. The used entries of one block name blocks of distinct sequence indices other than its own. Over all blocks of one sequence index, at most one distinct block of each other sequence index is named. On the last sequence index of each sample, the lists together name a block of every other index. `list_counts`: 0 for image blocks; at most 8. `image_blocks`: the blocks of the last sequence index of each sample are text blocks.
All inputs are finite; a program needn't handle non-finite values.
Results may differ from the reference program's by a relative error of at most 0.0043.
Values may be sent and summed in bfloat16 or wider, within the bound.
A program may use at most 128 MiB of HBM per device.

```python
import math
import jax
import jax.numpy as jnp
from jax import lax

QUERY_HEADS = 28
KEY_VALUE_HEADS = 4
HEAD_SIZE = 128
BLOCK_TOKENS = 128
REG = 64
LIST_ENTRIES = 8
BLK_DEV = 4
SAMPLE_COUNT = 4
TOK_DEV = 512
SAMPLE_BLOCKS = 32
SAMPLE_TOKENS = 4096
N_SEQ = 8


def activations(key):
    seeded = jax.random.fold_in(key, 11)
    key_queries, keys_for_keys = jax.random.split(seeded, 2)
    key_region = jnp.clip(jax.random.normal(keys_for_keys, (SAMPLE_COUNT, SAMPLE_TOKENS, KEY_VALUE_HEADS, HEAD_SIZE), jnp.float32), -6.0, 6.0)
    query_field = jnp.clip(jax.random.normal(key_queries, (SAMPLE_COUNT, SAMPLE_TOKENS, QUERY_HEADS, HEAD_SIZE), jnp.float32), -6.0, 6.0)
    query_out = query_field.reshape(SAMPLE_COUNT, SAMPLE_TOKENS, QUERY_HEADS * HEAD_SIZE).astype(jnp.bfloat16)
    key_output = key_region.reshape(SAMPLE_COUNT, SAMPLE_TOKENS, KEY_VALUE_HEADS * HEAD_SIZE).astype(jnp.bfloat16)
    return (query_out, key_output)


def draw_queries(key, part):
    return activations(key)[0]


def draw_keys(key, part):
    return activations(key)[1]


def layout(key):
    seeded = jax.random.fold_in(key, 7)
    key_kinds, key_chosen, key_order, key_counts = jax.random.split(seeded, 4)
    block_ids = jnp.arange(SAMPLE_BLOCKS, dtype=jnp.int32)
    block_device = block_ids // BLK_DEV
    local_ids = block_ids % BLK_DEV
    last_device = N_SEQ - 1
    kinds = (jax.random.randint(key_kinds, (SAMPLE_COUNT, SAMPLE_BLOCKS), 0, 4, jnp.int32) == 0).astype(jnp.int32)
    kinds = jnp.where(block_device[None, :] == last_device, 0, kinds)
    chosen = jax.random.randint(key_chosen, (SAMPLE_COUNT, N_SEQ, N_SEQ), 0, BLK_DEV, jnp.int32)
    owner_ids = jnp.arange(N_SEQ, dtype=jnp.int32)
    ranking = jax.random.randint(key_order, (SAMPLE_COUNT, SAMPLE_BLOCKS, N_SEQ), 0, 2 ** 16, jnp.int32) * N_SEQ + owner_ids
    ranking = jnp.where(owner_ids[None, None, :] != block_device[None, :, None], ranking, 2 ** 30)
    ordered = jnp.argsort(ranking, axis=-1)[..., :LIST_ENTRIES].astype(jnp.int32)
    slot_ids = jnp.arange(LIST_ENTRIES, dtype=jnp.int32)
    full_count = min(LIST_ENTRIES, N_SEQ - 1)
    cyclic = (local_ids[:, None] * full_count + slot_ids[None, :]) % (N_SEQ - 1)
    is_last = block_device == last_device
    ordered = jnp.where(is_last[None, :, None], cyclic[None], ordered)
    counts = full_count - jax.random.randint(key_counts, (SAMPLE_COUNT, SAMPLE_BLOCKS), 0, 3, jnp.int32)
    counts = jnp.where(is_last[None, :], full_count, counts)
    counts = jnp.where(kinds == 1, 0, counts)
    chosen_rows = chosen[:, block_device, :]
    picked = jnp.take_along_axis(chosen_rows, ordered, axis=2)
    list_ids = ordered * BLK_DEV + picked
    list_ids = jnp.where(slot_ids[None, None, :] < counts[..., None], list_ids, 0)
    return (list_ids.astype(jnp.int32), counts.astype(jnp.int32), kinds.astype(jnp.int32))


def draw_block_lists(key, part):
    return layout(key)[0]


def draw_list_counts(key, part):
    return layout(key)[1]


def draw_image_blocks(key, part):
    return layout(key)[2]


def place_ends(result, key, smallest, high):
    index_at = [jax.random.randint(jax.random.fold_in(key, axis), (), 0, length) for axis, length in enumerate(result.shape)]
    widest = result.shape.index(max(result.shape))
    beside = index_at[:widest] + [(index_at[widest] + 1) % result.shape[widest]] + index_at[widest + 1:]
    return result.at[tuple(index_at)].set(smallest).at[tuple(beside)].set(high)


def shard_levels(own_key, shape, cuts, low, high):
    gain = 1.0
    for dim, blocks in cuts:
        heights = jax.random.uniform(jax.random.fold_in(jax.random.fold_in(own_key, 6), dim), (blocks,), jnp.float32, low / len(cuts), high / len(cuts))
        gain = gain * jnp.repeat(jnp.exp(heights), shape[dim] // blocks).reshape((-1,) + (1,) * (len(shape) - 1 - dim))
    return gain


def normal_values(key, extent, width, most, pieces=(), kind=jnp.bfloat16):
    drawn = width * jax.random.normal(key, extent, jnp.float32)
    if pieces:
        drawn = drawn * shard_levels(key, extent, pieces, -0.22, 0.18)
    return jnp.clip(drawn, -most, most).astype(kind)


def setup_inputs(seed: int = 0) -> dict:
    splits = jax.random.split(jax.random.key(seed), 8)
    return {
        "queries": draw_queries(jax.random.fold_in(splits[7], 71), 0),
        "keys": draw_keys(jax.random.fold_in(splits[7], 71), 0),
        "values": normal_values(splits[2], (SAMPLE_COUNT, SAMPLE_TOKENS, KEY_VALUE_HEADS * HEAD_SIZE), 1.0, 6.0, ((0, 4), (1, 8))),
        "reg_owner": place_ends(jax.random.randint(splits[3], (SAMPLE_COUNT,), 0, N_SEQ), jax.random.fold_in(splits[3], 1), 0, N_SEQ - 1).astype(jnp.int32),
        "block_lists": draw_block_lists(jax.random.fold_in(splits[7], 71), 0),
        "list_counts": draw_list_counts(jax.random.fold_in(splits[7], 71), 0),
        "image_blocks": draw_image_blocks(jax.random.fold_in(splits[7], 71), 0),
    }


very_low = -1e+30

def group_part(query_row_list, key_row_list, value_row_list, visible):
    head_grouped = query_row_list.astype(jnp.float32).reshape(BLOCK_TOKENS, KEY_VALUE_HEADS, QUERY_HEADS // KEY_VALUE_HEADS, HEAD_SIZE)
    per_head_keys = key_row_list.astype(jnp.float32).reshape(-1, KEY_VALUE_HEADS, HEAD_SIZE)
    per_head_values = value_row_list.astype(jnp.float32).reshape(-1, KEY_VALUE_HEADS, HEAD_SIZE)
    scores = jnp.einsum('qhgd,khd->hgqk', head_grouped, per_head_keys) / math.sqrt(HEAD_SIZE)
    scores = jnp.where(visible, scores, very_low)
    maxima = lax.optimization_barrier(jnp.max(scores, axis=-1))
    weights = jnp.where(visible, jnp.exp(scores - maxima[..., None]), 0.0)
    totals = lax.optimization_barrier(jnp.sum(weights, axis=-1))
    rounded = lax.optimization_barrier(weights.astype(jnp.bfloat16)).astype(jnp.float32)
    partial_value = jnp.einsum('hgqk,khd->hgqd', rounded, per_head_values)
    return (maxima, totals, partial_value)

def combine(parts):
    top_score = jnp.maximum(jnp.maximum(parts[0][0], parts[1][0]), parts[2][0])
    numerator = jnp.zeros(parts[0][2].shape, jnp.float32)
    denominator = jnp.zeros(parts[0][1].shape, jnp.float32)
    for maxima, totals, partial_value in parts:
        rescale = jnp.exp(maxima - top_score)
        numerator = numerator + rescale[..., None] * partial_value
        denominator = denominator + rescale * totals
    merged = numerator / denominator[..., None]
    return merged.transpose(2, 0, 1, 3).reshape(merged.shape[2], -1)

def reference(queries, keys, values, reg_owner, block_lists, list_counts, image_blocks):
    outputs = []
    row_ids = jnp.arange(BLOCK_TOKENS)
    slot_rows = jnp.arange(LIST_ENTRIES * BLOCK_TOKENS) // BLOCK_TOKENS
    for sample in range(SAMPLE_COUNT):
        query_all = queries[sample]
        every_key = keys[sample]
        every_value = values[sample]
        blocked_keys = every_key.reshape(SAMPLE_BLOCKS, BLOCK_TOKENS, KEY_VALUE_HEADS * HEAD_SIZE)
        blocked_values = every_value.reshape(SAMPLE_BLOCKS, BLOCK_TOKENS, KEY_VALUE_HEADS * HEAD_SIZE)
        reg_start = (reg_owner[sample] * TOK_DEV).astype(jnp.int32)
        reg_keys = lax.dynamic_slice_in_dim(every_key, reg_start, REG, 0)
        reg_values = lax.dynamic_slice_in_dim(every_value, reg_start, REG, 0)
        sample_lists = block_lists[sample]
        sample_counts = list_counts[sample]
        sample_image = image_blocks[sample]

        def one_block(block_id):
            row_start = (block_id * BLOCK_TOKENS).astype(jnp.int32)
            query_row_list = lax.dynamic_slice_in_dim(query_all, row_start, BLOCK_TOKENS, 0)
            own_keys = lax.dynamic_slice_in_dim(every_key, row_start, BLOCK_TOKENS, 0)
            own_values = lax.dynamic_slice_in_dim(every_value, row_start, BLOCK_TOKENS, 0)
            listed_block_index = sample_lists[block_id]
            remote_keys = blocked_keys[listed_block_index].reshape(LIST_ENTRIES * BLOCK_TOKENS, KEY_VALUE_HEADS * HEAD_SIZE)
            remote_values = blocked_values[listed_block_index].reshape(LIST_ENTRIES * BLOCK_TOKENS, KEY_VALUE_HEADS * HEAD_SIZE)
            reg_visible = jnp.ones((BLOCK_TOKENS, REG), bool)
            own_visible = (row_ids[None, :] <= row_ids[:, None]) | (sample_image[block_id] == 1)
            far_visible = jnp.broadcast_to(slot_rows[None, :] < sample_counts[block_id], (BLOCK_TOKENS, LIST_ENTRIES * BLOCK_TOKENS))
            parts = [group_part(query_row_list, reg_keys, reg_values, reg_visible), group_part(query_row_list, own_keys, own_values, own_visible), group_part(query_row_list, remote_keys, remote_values, far_visible)]
            return combine(parts).astype(jnp.bfloat16)
        blocks_out = lax.map(one_block, jnp.arange(SAMPLE_BLOCKS, dtype=jnp.int32))
        outputs.append(blocks_out.reshape(SAMPLE_TOKENS, QUERY_HEADS * HEAD_SIZE))
    return jnp.stack(outputs)
```

```python
import functools
import math

import jax
import jax.numpy as jnp
from jax import lax
from jax.experimental import pallas as pl
from jax.experimental.pallas import tpu as pltpu
from jax.sharding import PartitionSpec as P

KEY_VALUE_HEADS = 4
HEAD_SIZE = 128
REG = 64
CHUNKS = 8
SUMS = 16
UNITS = 4

hidden = -1e30
score_gain = math.log2(math.e) / math.sqrt(HEAD_SIZE)
bf = jnp.bfloat16
f32 = jnp.float32


def stage_list(devices):
    if devices == 8:
        return [(1, 2, 4, 3, 5, 6, 7)]
    rest = list(range(1, devices))
    return [tuple(rest[i : i + 7]) for i in range(0, len(rest), 7)]


def split(keys):
    scaled = keys.astype(f32) * score_gain
    high = scaled.astype(bf)
    low = (scaled - high.astype(f32)).astype(bf)
    return high, low


def kernel(
    devices,
    lists_hbm,
    counts_hbm,
    image_hbm,
    owner_hbm,
    q_hbm,
    k_hbm,
    v_hbm,
    out_ref,
    lists_ref,
    counts_ref,
    image_ref,
    owner_ref,
    q_all,
    k_all,
    v_all,
    vt_own,
    need_out,
    need_in,
    chunk_out,
    chunk_in,
    reg_out,
    reg_in,
    x_out,
    x_in,
    acc,
    top,
    shown,
    own_mask,
    kk,
    vt,
    s_a,
    s_b,
    small_sem,
    local_sem,
    q_sem,
    send_need,
    recv_need,
    send_chunk,
    recv_chunk,
    send_reg,
    recv_reg,
    send_x,
    recv_x,
):
    me = lax.axis_index("seq")
    blocks, slots = lists_ref.shape
    rows = k_hbm.shape[1]
    heads = q_hbm.shape[1] // HEAD_SIZE
    group = heads // KEY_VALUE_HEADS
    chunk_rows = 2 * REG // CHUNKS
    peers = range(1, devices)
    wide = UNITS * rows
    steps = blocks * group // UNITS

    def peer(k):
        return me ^ k

    small = [
        pltpu.make_async_copy(lists_hbm, lists_ref, small_sem.at[0]),
        pltpu.make_async_copy(counts_hbm, counts_ref, small_sem.at[1]),
        pltpu.make_async_copy(image_hbm, image_ref, small_sem.at[2]),
        pltpu.make_async_copy(owner_hbm, owner_ref, small_sem.at[3]),
    ]
    for copy in small:
        copy.start()
    k_copy = pltpu.make_async_copy(k_hbm, k_all, local_sem.at[0])
    v_copy = pltpu.make_async_copy(v_hbm, v_all, local_sem.at[1])
    k_copy.start()
    v_copy.start()
    barrier = pltpu.get_barrier_semaphore()
    for k in peers:
        pl.semaphore_signal(barrier, inc=1, device_id={"seq": peer(k)})

    def q_copy(b):
        span = pl.ds(pl.multiple_of(b * rows, rows), rows)
        return pltpu.make_async_copy(q_hbm.at[span], q_all.at[span], q_sem.at[b])

    for b in range(blocks):
        q_copy(b).start()

    for copy in small:
        copy.wait()
    lane = lax.broadcasted_iota(jnp.int32, (8, 128), 1)
    wanted = jnp.zeros((8, 128), jnp.int32)
    for b in range(blocks):
        count = counts_ref[b]
        for t in range(slots):
            entry = lists_ref[b, t]
            source = jnp.where(t < count, lax.div(entry, blocks), -1)
            wanted = jnp.where(lane == source, lax.rem(entry, blocks), wanted)
    need_out[...] = wanted
    k_copy.wait()
    v_copy.wait()
    for c in range(CHUNKS):
        whole = k_all if c < CHUNKS // 2 else v_all
        start = (c % (CHUNKS // 2)) * chunk_rows
        chunk_out[c] = whole[0, start : start + chunk_rows]
    pl.semaphore_wait(barrier, devices - 1)

    def need_copy(k):
        return pltpu.make_async_remote_copy(
            need_out, need_in.at[k], send_need.at[k], recv_need.at[k], device_id={"seq": peer(k)}
        )

    def chunk_copy(k):
        return pltpu.make_async_remote_copy(
            chunk_out.at[lax.rem(peer(k), CHUNKS)],
            chunk_in.at[me],
            send_chunk.at[k],
            recv_chunk.at[k],
            device_id={"seq": peer(k)},
        )

    def reg_copy(k):
        return pltpu.make_async_remote_copy(
            reg_out, reg_in.at[me], send_reg.at[k], recv_reg.at[k], device_id={"seq": peer(k)}
        )

    def x_copy(k, g):
        return pltpu.make_async_remote_copy(
            x_out.at[k, g], x_in.at[k, g], send_x.at[k, g], recv_x.at[k, g], device_id={"seq": peer(k)}
        )

    order = list(reversed(peers))
    for k in order:
        need_copy(k).start()
    for k in order:
        chunk_copy(k).start()
    chunk_in[me] = chunk_out[lax.rem(me, CHUNKS)]

    for b in range(blocks):
        for g in range(KEY_VALUE_HEADS):
            column = slice(g * HEAD_SIZE, (g + 1) * HEAD_SIZE)
            vt_own[b, g, :HEAD_SIZE] = v_all[b, :, column].T
            vt_own[b, g, HEAD_SIZE:] = jnp.ones((SUMS, rows), bf)

    stages = stage_list(devices)

    for k in peers:
        need_copy(k).wait_recv()
    for group_of in stages:
        for k in group_of:
            row = need_in[k]
            pick = jnp.sum(jnp.where(lane[:1] == me, row[:1], 0))
            for g in range(KEY_VALUE_HEADS):
                columns = slice(g * HEAD_SIZE, (g + 1) * HEAD_SIZE)
                x_out[k, g, :rows] = k_all[pick, :, columns]
                x_out[k, g, rows:] = vt_own[pick, g, :HEAD_SIZE]
            x_copy(k, 0).start()
    for k in peers:
        chunk_copy(k).wait_recv()
    mine = chunk_in[owner_ref[0]]
    reg_out[...] = mine
    reg_in[me] = mine
    for k in order:
        reg_copy(k).start()
    for group_of in stages:
        for g in range(1, KEY_VALUE_HEADS):
            for k in group_of:
                x_copy(k, g).start()

    for k in peers:
        source = peer(k)
        for b in range(blocks):
            count = counts_ref[b]
            seen = jnp.int32(0)
            for t in range(slots):
                entry = lists_ref[b, t]
                hit = jnp.logical_and(lax.div(entry, blocks) == source, t < count)
                seen = jnp.where(hit, 1, seen)
            value = jnp.where(seen == 1, 0.0, hidden)
            shown[k, :, b * group * rows : (b + 1) * group * rows] = jnp.full((8, group * rows), value)

    key_side = lax.broadcasted_iota(jnp.int32, (rows, rows), 0)
    row_side = lax.broadcasted_iota(jnp.int32, (rows, rows), 1)
    for b in range(blocks):
        shut = jnp.where(image_ref[b] == 1, 0.0, hidden)
        own_mask[b] = jnp.where(key_side <= row_side, 0.0, shut)
    vt[HEAD_SIZE:] = jnp.ones((SUMS, vt.shape[1]), bf)

    nt = (((1,), (1,)), ((), ()))

    def own_step(i, carry):
        b = i // KEY_VALUE_HEADS
        g = lax.rem(i, KEY_VALUE_HEADS)

        @pl.when(g == 0)
        def _():
            q_copy(b).wait()

        column = pl.ds(pl.multiple_of(g * HEAD_SIZE, HEAD_SIZE), HEAD_SIZE)
        row_span = pl.ds(pl.multiple_of(b * rows, rows), rows)
        high, low = split(k_all[b, :, column])
        both = jnp.concatenate([high, low], axis=1)
        mask = own_mask[b]
        query = jnp.concatenate(
            [
                q_all[row_span, pl.ds(pl.multiple_of((g * group + h) * HEAD_SIZE, HEAD_SIZE), HEAD_SIZE)]
                for h in range(group)
            ],
            axis=0,
        )
        query = jnp.concatenate([query, query], axis=1)
        scores = lax.dot_general(both, query, nt, preferred_element_type=f32)
        scores = scores + jnp.concatenate([mask] * group, axis=1)
        best = jnp.max(scores, axis=0, keepdims=True)
        weights = jnp.exp2(scores - best).astype(bf)
        product = jnp.dot(vt_own[b, g], weights, preferred_element_type=f32)
        place = pl.ds(pl.multiple_of(b * group * rows, rows), group * rows)
        acc[g, :, place] = product[: HEAD_SIZE + 8]
        top[g, :, place] = jnp.broadcast_to(best, (8, group * rows))
        return carry

    lax.fori_loop(0, blocks * KEY_VALUE_HEADS, own_step, 0)

    for k in peers:
        reg_copy(k).wait_recv()

    half = CHUNKS // 2

    def far_group(g, carry, stage):
        first, last = stage == stages[0], stage == stages[-1]
        total = len(stage) * rows + (REG if first else 0)
        for k in stage:
            x_copy(k, g).wait_recv()
        for n, k in enumerate(stage):
            high, low = split(x_in[k, g, :rows])
            kk[n * rows : (n + 1) * rows, :HEAD_SIZE] = high
            kk[n * rows : (n + 1) * rows, HEAD_SIZE:] = low
            vt[:HEAD_SIZE, n * rows : (n + 1) * rows] = x_in[k, g, rows:]
        if first:
            column = pl.ds(pl.multiple_of(g * HEAD_SIZE, HEAD_SIZE), HEAD_SIZE)
            begin = len(stage) * rows
            high, low = split(reg_in[pl.ds(0, half), :, column].reshape(REG, HEAD_SIZE))
            kk[begin : begin + REG, :HEAD_SIZE] = high
            kk[begin : begin + REG, HEAD_SIZE:] = low
            vt[:HEAD_SIZE, begin : begin + REG] = reg_in[pl.ds(half, half), :, column].reshape(REG, HEAD_SIZE).T

        def unit(j, n):
            u = j * UNITS + n
            b = lax.div(u, group)
            h = lax.rem(u, group)
            row_span = pl.ds(pl.multiple_of(b * rows, rows), rows)
            column = pl.ds(pl.multiple_of((g * group + h) * HEAD_SIZE, HEAD_SIZE), HEAD_SIZE)
            return row_span, column

        def score(j, s_ref):
            query = jnp.concatenate([q_all[unit(j, n)] for n in range(UNITS)], axis=0)
            query = jnp.concatenate([query, query], axis=1)
            s_ref[:total] = lax.dot_general(kk[:total], query, nt, preferred_element_type=f32)

        def merge(j, s_ref):
            place = pl.ds(pl.multiple_of(j * wide, wide), wide)
            before = top[g, :, place]
            best = before
            for n, k in enumerate(stage):
                block = s_ref[n * rows : (n + 1) * rows].reshape(rows // 8, 8, wide)
                best = jnp.maximum(best, jnp.max(block, axis=0) + shown[k, :, place])
            if first:
                block = s_ref[len(stage) * rows : total].reshape(REG // 8, 8, wide)
                best = jnp.maximum(best, jnp.max(block, axis=0))
            best = jnp.broadcast_to(jnp.max(best, axis=0, keepdims=True), (8, wide))
            parts = []
            for n, k in enumerate(stage):
                shift = shown[k, :, place] - best
                block = s_ref[n * rows : (n + 1) * rows].reshape(rows // 8, 8, wide)
                parts.append(jnp.exp2(block + shift[None]).reshape(rows, wide).astype(bf))
            if first:
                block = s_ref[len(stage) * rows : total].reshape(REG // 8, 8, wide)
                parts.append(jnp.exp2(block - best[None]).reshape(REG, wide).astype(bf))
            weights = jnp.concatenate(parts, axis=0)
            product = jnp.dot(vt[:, :total], weights, preferred_element_type=f32)[: HEAD_SIZE + 8]
            scale = jnp.exp2(before - best)
            product = product.reshape(HEAD_SIZE // 8 + 1, 8, wide)
            product = product + acc[g, :, place].reshape(HEAD_SIZE // 8 + 1, 8, wide) * scale[None]
            if last:
                share = 1.0 / product[HEAD_SIZE // 8]
                merged = (product[: HEAD_SIZE // 8] * share[None]).reshape(HEAD_SIZE, wide)
                for n in range(UNITS):
                    one = merged[:, n * rows : (n + 1) * rows].T
                    out_ref[unit(j, n)] = one.astype(out_ref.dtype)
            else:
                acc[g, :, place] = product.reshape(HEAD_SIZE + 8, wide)
                top[g, :, place] = best

        score(0, s_a)

        def pair(i, carry):
            score(2 * i + 1, s_b)
            merge(2 * i, s_a)
            score(2 * i + 2, s_a)
            merge(2 * i + 1, s_b)
            return carry

        pairs = (steps - 1) // 2
        lax.fori_loop(0, pairs, pair, 0)
        if steps % 2 == 0:
            score(steps - 1, s_b)
            merge(steps - 2, s_a)
            merge(steps - 1, s_b)
        else:
            merge(steps - 1, s_a)
        return carry

    for stage in stages:
        lax.fori_loop(0, KEY_VALUE_HEADS, functools.partial(far_group, stage=stage), 0)

    for k in peers:
        need_copy(k).wait_send()
        chunk_copy(k).wait_send()
        reg_copy(k).wait_send()
        for g in range(KEY_VALUE_HEADS):
            x_copy(k, g).wait_send()


def per_device(queries, keys, values, reg_owner, block_lists, list_counts, image_blocks):
    devices = lax.axis_size("seq")
    tokens, width = queries.shape[1:]
    kv_width = keys.shape[2]
    blocks, slots = block_lists.shape[1:]
    rows = tokens // blocks
    chunk_rows = 2 * REG // CHUNKS
    spread = width // kv_width * tokens
    far = max(len(stage) for stage in stage_list(devices)) * rows + REG
    dma = pltpu.SemaphoreType.DMA
    pinned = functools.partial(pltpu.with_memory_space_constraint, memory_space=pltpu.HBM)
    anywhere = pl.BlockSpec(memory_space=pltpu.HBM)
    out = pl.pallas_call(
        functools.partial(kernel, devices),
        out_shape=jax.ShapeDtypeStruct((tokens, width), bf),
        in_specs=[anywhere] * 7,
        out_specs=pl.BlockSpec(memory_space=pltpu.VMEM),
        scratch_shapes=[
            pltpu.SMEM((blocks, slots), jnp.int32),
            pltpu.SMEM((blocks,), jnp.int32),
            pltpu.SMEM((blocks,), jnp.int32),
            pltpu.SMEM((1,), jnp.int32),
            pltpu.VMEM((tokens, width), bf),
            pltpu.VMEM((blocks, rows, kv_width), bf),
            pltpu.VMEM((blocks, rows, kv_width), bf),
            pltpu.VMEM((blocks, KEY_VALUE_HEADS, HEAD_SIZE + SUMS, rows), bf),
            pltpu.VMEM((8, 128), jnp.int32),
            pltpu.VMEM((devices, 8, 128), jnp.int32),
            pltpu.VMEM((CHUNKS, chunk_rows, kv_width), bf),
            pltpu.VMEM((devices, chunk_rows, kv_width), bf),
            pltpu.VMEM((chunk_rows, kv_width), bf),
            pltpu.VMEM((devices, chunk_rows, kv_width), bf),
            pltpu.VMEM((devices, KEY_VALUE_HEADS, 2 * rows, HEAD_SIZE), bf),
            pltpu.VMEM((devices, KEY_VALUE_HEADS, 2 * rows, HEAD_SIZE), bf),
            pltpu.VMEM((KEY_VALUE_HEADS, HEAD_SIZE + 8, spread), f32),
            pltpu.VMEM((KEY_VALUE_HEADS, 8, spread), f32),
            pltpu.VMEM((devices, 8, spread), f32),
            pltpu.VMEM((blocks, rows, rows), f32),
            pltpu.VMEM((far, 2 * HEAD_SIZE), bf),
            pltpu.VMEM((HEAD_SIZE + SUMS, far), bf),
            pltpu.VMEM((far, UNITS * rows), f32),
            pltpu.VMEM((far, UNITS * rows), f32),
            dma((4,)),
            dma((2,)),
            dma((blocks,)),
            dma((devices,)),
            dma((devices,)),
            dma((devices,)),
            dma((devices,)),
            dma((devices,)),
            dma((devices,)),
            dma((devices, KEY_VALUE_HEADS)),
            dma((devices, KEY_VALUE_HEADS)),
        ],
        compiler_params=pltpu.CompilerParams(
            collective_id=0, has_side_effects=True, vmem_limit_bytes=42 * 1024 * 1024 + devices * kv_width * rows * 4
        ),
    )(
        pinned(block_lists[0]),
        pinned(list_counts[0]),
        pinned(image_blocks[0]),
        reg_owner,
        pinned(queries[0]),
        pinned(keys.reshape(blocks, rows, kv_width)),
        pinned(values.reshape(blocks, rows, kv_width)),
    )
    return out[None]


def solution(mesh):
    placed = (
        P("samp", "seq", None),
        P("samp", "seq", None),
        P("samp", "seq", None),
        P("samp"),
        P("samp", "seq", None),
        P("samp", "seq"),
        P("samp", "seq"),
    )
    return jax.shard_map(
        per_device, mesh=mesh, in_specs=placed, out_specs=P("samp", "seq", None), check_vma=False
    )
```

```python
import functools
import math

import jax
import jax.numpy as jnp
from jax import lax
from jax.experimental import pallas as pl
from jax.experimental.pallas import tpu as pltpu
from jax.sharding import PartitionSpec as P

KEY_VALUE_HEADS = 4
HEAD_SIZE = 128
REG = 64
CHUNKS = 8
SUMS = 16
UNITS = 4

hidden = -1e30
score_gain = math.log2(math.e) / math.sqrt(HEAD_SIZE)
bf = jnp.bfloat16
f32 = jnp.float32


def stage_list(devices):
    if devices == 8:
        return [(1, 2, 4, 3, 5, 6, 7)]
    rest = list(range(1, devices))
    return [tuple(rest[i : i + 7]) for i in range(0, len(rest), 7)]


def last_list(devices):
    if devices == 8:
        return [(1, 2, 4, 3, 5), (6, 7)]
    return stage_list(devices)


def part_of(entry, blocks):
    if blocks & (blocks - 1):
        return lax.div(entry, blocks), lax.rem(entry, blocks)
    return lax.shift_right_logical(entry, blocks.bit_length() - 1), lax.bitwise_and(entry, blocks - 1)


def split(keys):
    scaled = keys.astype(f32) * score_gain
    high = scaled.astype(bf)
    low = (scaled - high.astype(f32)).astype(bf)
    return high, low


def kernel(
    devices,
    lists_hbm,
    counts_hbm,
    image_hbm,
    owner_hbm,
    q_hbm,
    k_hbm,
    v_hbm,
    out_ref,
    lists_ref,
    counts_ref,
    image_ref,
    owner_ref,
    q_all,
    k_all,
    v_all,
    vt_own,
    need_out,
    need_in,
    chunk_out,
    chunk_in,
    reg_out,
    reg_in,
    x_out,
    x_in,
    acc,
    top,
    shown,
    own_mask,
    kk,
    vt,
    s_a,
    s_b,
    m_a,
    m_b,
    small_sem,
    local_sem,
    q_sem,
    send_need,
    recv_need,
    send_chunk,
    recv_chunk,
    send_reg,
    recv_reg,
    send_x,
    recv_x,
):
    me = lax.axis_index("seq")
    blocks, slots = lists_ref.shape
    rows = k_hbm.shape[1]
    heads = q_hbm.shape[1] // HEAD_SIZE
    group = heads // KEY_VALUE_HEADS
    chunk_rows = 2 * REG // CHUNKS
    peers = range(1, devices)
    wide = UNITS * rows
    steps = blocks * group // UNITS

    def peer(k):
        return me ^ k

    small = [
        pltpu.make_async_copy(lists_hbm, lists_ref, small_sem.at[0]),
        pltpu.make_async_copy(counts_hbm, counts_ref, small_sem.at[1]),
        pltpu.make_async_copy(image_hbm, image_ref, small_sem.at[2]),
        pltpu.make_async_copy(owner_hbm, owner_ref, small_sem.at[3]),
    ]
    for copy in small:
        copy.start()
    k_copy = pltpu.make_async_copy(k_hbm, k_all, local_sem.at[0])
    v_copy = pltpu.make_async_copy(v_hbm, v_all, local_sem.at[1])
    k_copy.start()
    v_copy.start()
    barrier = pltpu.get_barrier_semaphore()
    for k in peers:
        pl.semaphore_signal(barrier, inc=1, device_id={"seq": peer(k)})

    def q_copy(b):
        span = pl.ds(pl.multiple_of(b * rows, rows), rows)
        return pltpu.make_async_copy(q_hbm.at[span], q_all.at[span], q_sem.at[b])

    for b in range(blocks):
        q_copy(b).start()

    for copy in small:
        copy.wait()
    lane = lax.broadcasted_iota(jnp.int32, (8, 128), 1)
    wanted = jnp.zeros((8, 128), jnp.int32)
    sources = []
    for b in range(blocks):
        count = counts_ref[b]
        sources.append([])
        for t in range(slots):
            source, local = part_of(lists_ref[b, t], blocks)
            source = jnp.where(t < count, source, -1)
            sources[b].append(source)
            wanted = jnp.where(lane == source, local, wanted)
    need_out[...] = wanted
    k_copy.wait()
    v_copy.wait()
    for c in range(CHUNKS):
        whole = k_all if c < CHUNKS // 2 else v_all
        start = (c % (CHUNKS // 2)) * chunk_rows
        chunk_out[c] = whole[0, start : start + chunk_rows]
    pl.semaphore_wait(barrier, devices - 1)

    def need_copy(k):
        return pltpu.make_async_remote_copy(
            need_out, need_in.at[k], send_need.at[k], recv_need.at[k], device_id={"seq": peer(k)}
        )

    def chunk_copy(k):
        return pltpu.make_async_remote_copy(
            chunk_out.at[lax.rem(peer(k), CHUNKS)],
            chunk_in.at[me],
            send_chunk.at[k],
            recv_chunk.at[k],
            device_id={"seq": peer(k)},
        )

    def reg_copy(k):
        return pltpu.make_async_remote_copy(
            reg_out, reg_in.at[me], send_reg.at[k], recv_reg.at[k], device_id={"seq": peer(k)}
        )

    def x_copy(k, g):
        return pltpu.make_async_remote_copy(
            x_out.at[k, g], x_in.at[k, g], send_x.at[k, g], recv_x.at[k, g], device_id={"seq": peer(k)}
        )

    order = list(reversed(peers))
    for k in order:
        need_copy(k).start()
    for k in order:
        chunk_copy(k).start()
    chunk_in[me] = chunk_out[lax.rem(me, CHUNKS)]

    for b in range(blocks):
        for g in range(KEY_VALUE_HEADS):
            column = slice(g * HEAD_SIZE, (g + 1) * HEAD_SIZE)
            vt_own[b, g, :HEAD_SIZE] = v_all[b, :, column].T
            vt_own[b, g, HEAD_SIZE:] = jnp.ones((SUMS, rows), bf)

    stages = stage_list(devices)

    for k in peers:
        need_copy(k).wait_recv()
    picks = {}
    for k in peers:
        row = need_in[k]
        picks[k] = jnp.sum(jnp.where(lane[:1] == me, row[:1], 0))

    def fill(k, g):
        columns = slice(g * HEAD_SIZE, (g + 1) * HEAD_SIZE)
        x_out[k, g, :rows] = k_all[picks[k], :, columns]
        x_out[k, g, rows:] = vt_own[picks[k], g, :HEAD_SIZE]

    for group_of in stages:
        for k in group_of:
            fill(k, 0)
            x_copy(k, 0).start()
    for k in peers:
        chunk_copy(k).wait_recv()
    mine = chunk_in[owner_ref[0]]
    reg_out[...] = mine
    reg_in[me] = mine
    for k in order:
        reg_copy(k).start()
    for g in range(1, KEY_VALUE_HEADS):
        for group_of in stages:
            for k in group_of:
                fill(k, g)
                x_copy(k, g).start()

    for k in peers:
        source = peer(k)
        for b in range(blocks):
            seen = functools.reduce(jnp.logical_or, [found == source for found in sources[b]])
            value = jnp.where(seen, 0.0, hidden)
            shown[k, :, b * group * rows : (b + 1) * group * rows] = jnp.full((8, group * rows), value)

    key_side = lax.broadcasted_iota(jnp.int32, (rows, rows), 0)
    row_side = lax.broadcasted_iota(jnp.int32, (rows, rows), 1)
    for b in range(blocks):
        shut = jnp.where(image_ref[b] == 1, 0.0, hidden)
        own_mask[b] = jnp.where(key_side <= row_side, 0.0, shut)
    vt[HEAD_SIZE:] = jnp.ones((SUMS, vt.shape[1]), bf)

    nt = (((1,), (1,)), ((), ()))

    def own_step(b, carry):
        q_copy(b).wait()
        row_span = pl.ds(pl.multiple_of(b * rows, rows), rows)
        place = pl.ds(pl.multiple_of(b * group * rows, rows), group * rows)
        mask = jnp.concatenate([own_mask[b]] * group, axis=1)

        def scored(g):
            high, low = split(k_all[b, :, g * HEAD_SIZE : (g + 1) * HEAD_SIZE])
            both = jnp.concatenate([high, low], axis=1)
            query = jnp.concatenate(
                [
                    q_all[row_span, (g * group + h) * HEAD_SIZE : (g * group + h + 1) * HEAD_SIZE]
                    for h in range(group)
                ],
                axis=0,
            )
            query = jnp.concatenate([query, query], axis=1)
            return lax.dot_general(both, query, nt, preferred_element_type=f32) + mask

        ahead = scored(0)
        for g in range(KEY_VALUE_HEADS):
            scores = ahead
            if g + 1 < KEY_VALUE_HEADS:
                ahead = scored(g + 1)
            best = jnp.max(scores, axis=0, keepdims=True)
            weights = jnp.exp2(scores - best).astype(bf)
            product = jnp.dot(vt_own[b, g], weights, preferred_element_type=f32)
            acc[g, :, place] = product[: HEAD_SIZE + 8]
            top[g, :, place] = jnp.broadcast_to(best, (8, group * rows))
        return carry

    lax.fori_loop(0, blocks, own_step, 0)

    for k in peers:
        reg_copy(k).wait_recv()

    half = CHUNKS // 2

    def far_stage(g, stage, first, last):
        total = len(stage) * rows + (REG if first else 0)
        for k in stage:
            x_copy(k, g).wait_recv()
        for n, k in enumerate(stage):
            high, low = split(x_in[k, g, :rows])
            kk[n * rows : (n + 1) * rows, :HEAD_SIZE] = high
            kk[n * rows : (n + 1) * rows, HEAD_SIZE:] = low
            vt[:HEAD_SIZE, n * rows : (n + 1) * rows] = x_in[k, g, rows:]
        if first:
            column = pl.ds(pl.multiple_of(g * HEAD_SIZE, HEAD_SIZE), HEAD_SIZE)
            begin = len(stage) * rows
            high, low = split(reg_in[pl.ds(0, half), :, column].reshape(REG, HEAD_SIZE))
            kk[begin : begin + REG, :HEAD_SIZE] = high
            kk[begin : begin + REG, HEAD_SIZE:] = low
            vt[:HEAD_SIZE, begin : begin + REG] = reg_in[pl.ds(half, half), :, column].reshape(REG, HEAD_SIZE).T

        pieces = [(n * rows, rows, k) for n, k in enumerate(stage)]
        if first:
            pieces.append((len(stage) * rows, REG, None))

        def unit(j, n):
            u = j * UNITS + n
            b, h = u // group, u % group
            column = pl.ds(pl.multiple_of((g * group + h) * HEAD_SIZE, HEAD_SIZE), HEAD_SIZE)
            return pl.ds(b * rows, rows), column

        def place_of(j):
            return pl.ds(j * wide, wide)

        def score(j, s_ref, m_ref):
            place = place_of(j)
            query = jnp.concatenate([q_all[unit(j, n)] for n in range(UNITS)], axis=0)
            query = jnp.concatenate([query, query], axis=1)
            scores = lax.dot_general(kk[:total], query, nt, preferred_element_type=f32)
            s_ref[:total] = scores
            best = top[g, :, place]
            for begin, size, k in pieces:
                block = jnp.max(scores[begin : begin + size].reshape(size // 8, 8, wide), axis=0)
                best = jnp.maximum(best, block if k is None else block + shown[k, :, place])
            m_ref[...] = jnp.broadcast_to(jnp.max(best, axis=0, keepdims=True), (8, wide))

        def merge(j, s_ref, m_ref):
            place = place_of(j)
            before = top[g, :, place]
            best = m_ref[...]
            product = None
            for c in range(0, len(pieces), 2):
                parts = []
                for begin, size, k in pieces[c : c + 2]:
                    shift = -best if k is None else shown[k, :, place] - best
                    block = s_ref[begin : begin + size].reshape(size // 8, 8, wide)
                    parts.append(jnp.exp2(block + shift[None]).reshape(size, wide).astype(bf))
                begin = pieces[c][0]
                weights = jnp.concatenate(parts, axis=0)
                more = jnp.dot(vt[:, begin : begin + weights.shape[0]], weights, preferred_element_type=f32)
                product = more if product is None else product + more
            product = product[: HEAD_SIZE + 8]
            scale = jnp.exp2(before - best)
            product = product.reshape(HEAD_SIZE // 8 + 1, 8, wide)
            product = product + acc[g, :, place].reshape(HEAD_SIZE // 8 + 1, 8, wide) * scale[None]
            if last:
                share = 1.0 / product[HEAD_SIZE // 8]
                merged = (product[: HEAD_SIZE // 8] * share[None]).reshape(HEAD_SIZE, wide).astype(bf)
                for n in range(UNITS):
                    out_ref[unit(j, n)] = merged[:, n * rows : (n + 1) * rows].T
            else:
                acc[g, :, place] = product.reshape(HEAD_SIZE + 8, wide)
                top[g, :, place] = best

        score(0, s_a, m_a)

        buffers = ((s_a, m_a), (s_b, m_b))
        for j in range(steps):
            if j + 1 < steps:
                score(j + 1, *buffers[(j + 1) % 2])
            merge(j, *buffers[j % 2])

    def far_group(g, carry, plan):
        for stage in plan:
            far_stage(g, stage, stage == plan[0], stage == plan[-1])
        return carry

    ends = last_list(devices)
    same = KEY_VALUE_HEADS - (ends != stages)
    lax.fori_loop(0, same, functools.partial(far_group, plan=stages), 0)
    for g in range(same, KEY_VALUE_HEADS):
        far_group(g, 0, ends)

    for k in peers:
        need_copy(k).wait_send()
        chunk_copy(k).wait_send()
        reg_copy(k).wait_send()
        for g in range(KEY_VALUE_HEADS):
            x_copy(k, g).wait_send()


def per_device(queries, keys, values, reg_owner, block_lists, list_counts, image_blocks):
    devices = lax.axis_size("seq")
    tokens, width = queries.shape[1:]
    kv_width = keys.shape[2]
    blocks, slots = block_lists.shape[1:]
    rows = tokens // blocks
    chunk_rows = 2 * REG // CHUNKS
    spread = width // kv_width * tokens
    far = max(len(stage) for stage in stage_list(devices)) * rows + REG
    dma = pltpu.SemaphoreType.DMA
    pinned = functools.partial(pltpu.with_memory_space_constraint, memory_space=pltpu.HBM)
    anywhere = pl.BlockSpec(memory_space=pltpu.HBM)
    out = pl.pallas_call(
        functools.partial(kernel, devices),
        out_shape=jax.ShapeDtypeStruct((tokens, width), bf),
        in_specs=[anywhere] * 7,
        out_specs=pl.BlockSpec(memory_space=pltpu.VMEM),
        scratch_shapes=[
            pltpu.SMEM((blocks, slots), jnp.int32),
            pltpu.SMEM((blocks,), jnp.int32),
            pltpu.SMEM((blocks,), jnp.int32),
            pltpu.SMEM((1,), jnp.int32),
            pltpu.VMEM((tokens, width), bf),
            pltpu.VMEM((blocks, rows, kv_width), bf),
            pltpu.VMEM((blocks, rows, kv_width), bf),
            pltpu.VMEM((blocks, KEY_VALUE_HEADS, HEAD_SIZE + SUMS, rows), bf),
            pltpu.VMEM((8, 128), jnp.int32),
            pltpu.VMEM((devices, 8, 128), jnp.int32),
            pltpu.VMEM((CHUNKS, chunk_rows, kv_width), bf),
            pltpu.VMEM((devices, chunk_rows, kv_width), bf),
            pltpu.VMEM((chunk_rows, kv_width), bf),
            pltpu.VMEM((devices, chunk_rows, kv_width), bf),
            pltpu.VMEM((devices, KEY_VALUE_HEADS, 2 * rows, HEAD_SIZE), bf),
            pltpu.VMEM((devices, KEY_VALUE_HEADS, 2 * rows, HEAD_SIZE), bf),
            pltpu.VMEM((KEY_VALUE_HEADS, HEAD_SIZE + 8, spread), f32),
            pltpu.VMEM((KEY_VALUE_HEADS, 8, spread), f32),
            pltpu.VMEM((devices, 8, spread), f32),
            pltpu.VMEM((blocks, rows, rows), f32),
            pltpu.VMEM((far, 2 * HEAD_SIZE), bf),
            pltpu.VMEM((HEAD_SIZE + SUMS, far), bf),
            pltpu.VMEM((far, UNITS * rows), f32),
            pltpu.VMEM((far, UNITS * rows), f32),
            pltpu.VMEM((8, UNITS * rows), f32),
            pltpu.VMEM((8, UNITS * rows), f32),
            dma((4,)),
            dma((2,)),
            dma((blocks,)),
            dma((devices,)),
            dma((devices,)),
            dma((devices,)),
            dma((devices,)),
            dma((devices,)),
            dma((devices,)),
            dma((devices, KEY_VALUE_HEADS)),
            dma((devices, KEY_VALUE_HEADS)),
        ],
        compiler_params=pltpu.CompilerParams(
            collective_id=0, has_side_effects=True, vmem_limit_bytes=42 * 1024 * 1024 + devices * kv_width * rows * 4
        ),
    )(
        pinned(block_lists[0]),
        pinned(list_counts[0]),
        pinned(image_blocks[0]),
        reg_owner,
        pinned(queries[0]),
        pinned(keys.reshape(blocks, rows, kv_width)),
        pinned(values.reshape(blocks, rows, kv_width)),
    )
    return out[None]


def solution(mesh):
    placed = (
        P("samp", "seq", None),
        P("samp", "seq", None),
        P("samp", "seq", None),
        P("samp"),
        P("samp", "seq", None),
        P("samp", "seq"),
        P("samp", "seq"),
    )
    return jax.shard_map(
        per_device, mesh=mesh, in_specs=placed, out_specs=P("samp", "seq", None), check_vma=False
    )
```

```python
import functools
import math

import jax
import jax.numpy as jnp
from jax import lax
from jax.experimental import pallas as pl
from jax.experimental.pallas import tpu as pltpu
from jax.sharding import PartitionSpec as P

KEY_VALUE_HEADS = 4
HEAD_SIZE = 128
REG = 64
CHUNKS = 8
SUMS = 16
UNITS = 4

hidden = -1e30
score_gain = math.log2(math.e) / math.sqrt(HEAD_SIZE)
bf = jnp.bfloat16
f32 = jnp.float32


def stage_list(devices):
    if devices == 8:
        return [(1, 2, 4, 3, 5), (6, 7)]
    rest = list(range(1, devices))
    return [tuple(rest[i : i + 7]) for i in range(0, len(rest), 7)]


def late_peers(devices):
    return stage_list(devices)[-1] if devices == 8 else ()


def part_of(entry, blocks):
    if blocks & (blocks - 1):
        return lax.div(entry, blocks), lax.rem(entry, blocks)
    return lax.shift_right_logical(entry, blocks.bit_length() - 1), lax.bitwise_and(entry, blocks - 1)


def split(keys):
    scaled = keys.astype(f32) * score_gain
    high = scaled.astype(bf)
    low = (scaled - high.astype(f32)).astype(bf)
    return high, low


def kernel(
    devices,
    lists_hbm,
    counts_hbm,
    image_hbm,
    owner_hbm,
    q_hbm,
    k_hbm,
    v_hbm,
    out_ref,
    lists_ref,
    counts_ref,
    image_ref,
    owner_ref,
    q_all,
    k_all,
    v_all,
    vt_own,
    need_out,
    need_in,
    chunk_out,
    chunk_in,
    reg_out,
    reg_in,
    x_out,
    x_in,
    acc,
    top,
    shown,
    own_mask,
    kk,
    vt,
    s_a,
    s_b,
    m_a,
    m_b,
    held,
    held_top,
    out_all,
    out_sem,
    small_sem,
    local_sem,
    q_sem,
    send_sem,
    recv_need,
    recv_sem,
    recv_x,
):
    me = lax.axis_index("seq")
    blocks, slots = lists_ref.shape
    rows = k_hbm.shape[1]
    heads = q_hbm.shape[1] // HEAD_SIZE
    group = heads // KEY_VALUE_HEADS
    chunk_rows = 2 * REG // CHUNKS
    peers = range(1, devices)
    wide = UNITS * rows
    steps = blocks * group // UNITS
    late = late_peers(devices)
    stages = stage_list(devices)

    def peer(k):
        return me ^ k

    small = [
        pltpu.make_async_copy(lists_hbm, lists_ref, small_sem.at[0]),
        pltpu.make_async_copy(counts_hbm, counts_ref, small_sem.at[1]),
        pltpu.make_async_copy(image_hbm, image_ref, small_sem.at[2]),
        pltpu.make_async_copy(owner_hbm, owner_ref, small_sem.at[3]),
    ]
    for copy in small:
        copy.start()
    k_copy = pltpu.make_async_copy(k_hbm, k_all, local_sem.at[0])
    v_copy = pltpu.make_async_copy(v_hbm, v_all, local_sem.at[1])
    k_copy.start()
    v_copy.start()
    barrier = pltpu.get_barrier_semaphore()
    for k in peers:
        pl.semaphore_signal(barrier, inc=1, device_id={"seq": peer(k)})

    def q_copy(b):
        span = pl.ds(pl.multiple_of(b * rows, rows), rows)
        return pltpu.make_async_copy(q_hbm.at[span], q_all.at[span], q_sem.at[b])

    for b in range(blocks):
        q_copy(b).start()

    for copy in small:
        copy.wait()
    lane = lax.broadcasted_iota(jnp.int32, (8, 128), 1)
    wanted = jnp.zeros((8, 128), jnp.int32)
    sources = []
    for b in range(blocks):
        count = counts_ref[b]
        sources.append([])
        for t in range(slots):
            source, local = part_of(lists_ref[b, t], blocks)
            source = jnp.where(t < count, source, -1)
            sources[b].append(source)
            wanted = jnp.where(lane == source, local, wanted)
    need_out[...] = wanted
    k_copy.wait()
    v_copy.wait()
    for c in range(CHUNKS):
        whole = k_all if c < CHUNKS // 2 else v_all
        start = (c % (CHUNKS // 2)) * chunk_rows
        chunk_out[c] = whole[0, start : start + chunk_rows]
    pl.semaphore_wait(barrier, devices - 1)

    def need_copy(k):
        return pltpu.make_async_remote_copy(
            need_out, need_in.at[k], send_sem.at[0], recv_need.at[k - 1], device_id={"seq": peer(k)}
        )

    def chunk_copy(k):
        return pltpu.make_async_remote_copy(
            chunk_out.at[lax.rem(peer(k), CHUNKS)],
            chunk_in.at[me],
            send_sem.at[1],
            recv_sem.at[0],
            device_id={"seq": peer(k)},
        )

    alike = range(2, devices, 2)

    def reg_copy(k):
        return pltpu.make_async_remote_copy(
            reg_out, reg_in.at[me], send_sem.at[2], recv_sem.at[1], device_id={"seq": peer(k)}
        )

    def pass_copy(k):
        return pltpu.make_async_remote_copy(
            reg_in.at[peer(k)], reg_in.at[peer(k)], send_sem.at[3], recv_sem.at[2], device_id={"seq": peer(1)}
        )

    def x_copy(k, g, part):
        span = pl.ds(part * rows, rows if k in late else 2 * rows)
        n = [k in stage for stage in stages].index(True) + part
        return pltpu.make_async_remote_copy(
            x_out.at[k, g, span], x_in.at[k, g, span], send_sem.at[4], recv_x.at[n, g], device_id={"seq": peer(k)}
        )

    def total(ref, kind, received):
        return pltpu.make_async_remote_copy(ref, ref, send_sem.at[kind], received, device_id={"seq": peer(1)})

    def arrive(stage, g, part):
        span = pl.ds(part * rows, rows if stage == late else 2 * rows)
        ref = x_in.at[pl.ds(min(stage), len(stage)), g, span]
        total(ref, 4, recv_x.at[stages.index(stage) + part, g]).wait_recv()

    order = list(reversed(peers))
    for k in order:
        need_copy(k).start()
    for k in order:
        chunk_copy(k).start()
    chunk_in[me] = chunk_out[lax.rem(me, CHUNKS)]

    for b in range(blocks):
        for g in range(KEY_VALUE_HEADS):
            column = slice(g * HEAD_SIZE, (g + 1) * HEAD_SIZE)
            vt_own[b, g, :HEAD_SIZE] = v_all[b, :, column].T
            vt_own[b, g, HEAD_SIZE:] = jnp.ones((SUMS, rows), bf)

    picks = {}

    def fill(k, g):
        columns = pl.ds(g * HEAD_SIZE, HEAD_SIZE)
        x_out[k, g, :rows] = k_all[picks[k], :, columns]
        x_out[k, g, rows:] = vt_own[picks[k], g, :HEAD_SIZE]

    def answer(k):
        need_copy(k).wait_recv()
        row = need_in[k]
        picks[k] = jnp.sum(jnp.where(lane[:1] == me, row[:1], 0))
        fill(k, 0)
        if k not in late:
            x_copy(k, 0, 0).start()

    everyone = [k for stage in stages for k in stage]
    for k in everyone[:3]:
        answer(k)
    total(chunk_in.at[pl.ds(0, devices - 1)], 1, recv_sem.at[0]).wait_recv()
    mine = chunk_in[owner_ref[0]]
    reg_out[...] = mine
    reg_in[me] = mine
    for k in reversed(alike):
        reg_copy(k).start()
    pass_copy(0).start()
    for k in everyone[3:]:
        answer(k)

    def send(g):
        for k in everyone:
            fill(k, g)
            x_copy(k, g, 0).start()
        for k in late:
            x_copy(k, g, 1).start()

    for k in peers:
        source = peer(k)
        for b in range(blocks):
            seen = functools.reduce(jnp.logical_or, [found == source for found in sources[b]])
            value = jnp.where(seen, 0.0, hidden)
            shown[k, :, b * group * rows : (b + 1) * group * rows] = jnp.full((8, group * rows), value)

    key_side = lax.broadcasted_iota(jnp.int32, (rows, rows), 0)
    row_side = lax.broadcasted_iota(jnp.int32, (rows, rows), 1)
    for b in range(blocks):
        shut = jnp.where(image_ref[b] == 1, 0.0, hidden)
        own_mask[b] = jnp.where(key_side <= row_side, 0.0, shut)
    vt[HEAD_SIZE:] = jnp.ones((SUMS, vt.shape[1]), bf)

    nt = (((1,), (1,)), ((), ()))

    def own_step(b, carry):
        @pl.when(b == 1)
        def _():
            for part in range(2):
                for k in late:
                    x_copy(k, 0, part).start()

        @pl.when(b == blocks - 1)
        def _():
            send(1)

        @pl.when(b == blocks - 1)
        def _():
            total(reg_in.at[pl.ds(0, len(alike))], 2, recv_sem.at[1]).wait_recv()
            for k in alike:
                pass_copy(k).start()

        q_copy(b).wait()
        row_span = pl.ds(pl.multiple_of(b * rows, rows), rows)
        place = pl.ds(pl.multiple_of(b * group * rows, rows), group * rows)
        mask = jnp.concatenate([own_mask[b]] * group, axis=1)

        def scored(g):
            own_keys = k_all[b, :, g * HEAD_SIZE : (g + 1) * HEAD_SIZE]
            query = jnp.concatenate(
                [
                    q_all[row_span, (g * group + h) * HEAD_SIZE : (g * group + h + 1) * HEAD_SIZE]
                    for h in range(group)
                ],
                axis=0,
            )
            return lax.dot_general(own_keys, query, nt, preferred_element_type=f32) * score_gain + mask

        ahead = scored(0)
        for g in range(KEY_VALUE_HEADS):
            scores = ahead
            if g + 1 < KEY_VALUE_HEADS:
                ahead = scored(g + 1)
            best = jnp.max(scores, axis=0, keepdims=True)
            weights = jnp.exp2(scores - best).astype(bf)
            product = jnp.dot(vt_own[b, g], weights, preferred_element_type=f32)
            acc[g, :, place] = product[: HEAD_SIZE + 8]
            top[g, :, place] = jnp.broadcast_to(best, (8, group * rows))
        return carry

    lax.fori_loop(0, blocks, own_step, 0)
    total(reg_in.at[pl.ds(0, devices // 2)], 3, recv_sem.at[2]).wait_recv()

    half = CHUNKS // 2

    def far_stage(g, stage, first, last):
        size_all = len(stage) * rows + (REG if first else 0)
        apart = stage == late
        arrive(stage, g, 0)
        if first:

            @pl.when(g < KEY_VALUE_HEADS - 2)
            def _():
                send(g + 2)

        for n, k in enumerate(stage):
            high, low = split(x_in[k, g, :rows])
            kk[n * rows : (n + 1) * rows, :HEAD_SIZE] = high
            kk[n * rows : (n + 1) * rows, HEAD_SIZE:] = low

        def load_values():
            for n, k in enumerate(stage):
                vt[:HEAD_SIZE, n * rows : (n + 1) * rows] = x_in[k, g, rows:]

        if not apart:
            load_values()
        if first:
            column = pl.ds(pl.multiple_of(g * HEAD_SIZE, HEAD_SIZE), HEAD_SIZE)
            begin = len(stage) * rows
            high, low = split(reg_in[pl.ds(0, half), :, column].reshape(REG, HEAD_SIZE))
            kk[begin : begin + REG, :HEAD_SIZE] = high
            kk[begin : begin + REG, HEAD_SIZE:] = low
            vt[:HEAD_SIZE, begin : begin + REG] = reg_in[pl.ds(half, half), :, column].reshape(REG, HEAD_SIZE).T

        pieces = [(n * rows, rows, k) for n, k in enumerate(stage)]
        if first:
            pieces.append((len(stage) * rows, REG, None))

        def unit(j, n):
            u = j * UNITS + n
            b, h = u // group, u % group
            column = pl.ds(pl.multiple_of((g * group + h) * HEAD_SIZE, HEAD_SIZE), HEAD_SIZE)
            return pl.ds(b * rows, rows), column

        def place_of(j):
            return pl.ds(j * wide, wide)

        def score(j, s_ref, m_ref):
            place = place_of(j)
            query = jnp.concatenate([q_all[unit(j, n)] for n in range(UNITS)], axis=0)
            query = jnp.concatenate([query, query], axis=1)
            scores = lax.dot_general(kk[:size_all], query, nt, preferred_element_type=f32)
            s_ref[:size_all] = scores
            best = top[g, :, place]
            for begin, size, k in pieces:
                block = jnp.max(scores[begin : begin + size].reshape(size // 8, 8, wide), axis=0)
                best = jnp.maximum(best, block if k is None else block + shown[k, :, place])
            m_ref[...] = jnp.broadcast_to(jnp.max(best, axis=0, keepdims=True), (8, wide))

        def weigh(j, s_ref, best, chosen):
            parts = []
            for begin, size, k in chosen:
                shift = -best if k is None else shown[k, :, place_of(j)] - best
                block = s_ref[begin : begin + size].reshape(size // 8, 8, wide)
                parts.append(jnp.exp2(block + shift[None]).reshape(size, wide).astype(bf))
            return jnp.concatenate(parts, axis=0)

        def finish(j, product, best):
            place = place_of(j)
            scale = jnp.exp2(top[g, :, place] - best)
            product = product[: HEAD_SIZE + 8].reshape(HEAD_SIZE // 8 + 1, 8, wide)
            product = product + acc[g, :, place].reshape(HEAD_SIZE // 8 + 1, 8, wide) * scale[None]
            if last:
                share = 1.0 / product[HEAD_SIZE // 8]
                merged = (product[: HEAD_SIZE // 8] * share[None]).reshape(HEAD_SIZE, wide).astype(bf)
                for n in range(UNITS):
                    out_all[unit(j, n)] = merged[:, n * rows : (n + 1) * rows].T
            else:
                acc[g, :, place] = product.reshape(HEAD_SIZE + 8, wide)
                top[g, :, place] = best

        def merge(j, s_ref, m_ref):
            best = m_ref[...]
            product = None
            for c in range(0, len(pieces), 2):
                begin = pieces[c][0]
                weights = weigh(j, s_ref, best, pieces[c : c + 2])
                more = jnp.dot(vt[:, begin : begin + weights.shape[0]], weights, preferred_element_type=f32)
                product = more if product is None else product + more
            finish(j, product, best)

        def keep(j, s_ref, m_ref):
            best = m_ref[...]
            held[:, place_of(j)] = weigh(j, s_ref, best, pieces)
            held_top[:, place_of(j)] = best

        score(0, s_a, m_a)
        buffers = ((s_a, m_a), (s_b, m_b))
        for j in range(steps):
            if j + 1 < steps:
                score(j + 1, *buffers[(j + 1) % 2])
            (keep if apart else merge)(j, *buffers[j % 2])
        if apart:
            arrive(stage, g, 1)
            load_values()
            for j in range(steps):
                product = jnp.dot(vt[:, :size_all], held[:, place_of(j)], preferred_element_type=f32)
                finish(j, product, held_top[:, place_of(j)])

    def out_copy(g):
        span = pl.ds(pl.multiple_of(g * group * HEAD_SIZE, HEAD_SIZE), group * HEAD_SIZE)
        return pltpu.make_async_copy(out_all.at[:, span], out_ref.at[:, span], out_sem.at[0])

    def far_group(g, carry):
        for stage in stages:
            far_stage(g, stage, stage == stages[0], stage == stages[-1])
        out_copy(g).start()
        return carry

    lax.fori_loop(0, KEY_VALUE_HEADS, far_group, 0)

    pltpu.make_async_copy(out_all, out_ref, out_sem.at[0]).wait()
    total(need_in.at[pl.ds(0, devices - 1)], 0, recv_sem.at[0]).wait_send()
    total(chunk_in.at[pl.ds(0, devices - 1)], 1, recv_sem.at[0]).wait_send()
    total(reg_in.at[pl.ds(0, len(alike))], 2, recv_sem.at[1]).wait_send()
    total(reg_in.at[pl.ds(0, devices // 2)], 3, recv_sem.at[2]).wait_send()
    total(x_out.at[pl.ds(1, devices - 1)], 4, recv_sem.at[0]).wait_send()


def per_device(queries, keys, values, reg_owner, block_lists, list_counts, image_blocks):
    devices = lax.axis_size("seq")
    tokens, width = queries.shape[1:]
    kv_width = keys.shape[2]
    blocks, slots = block_lists.shape[1:]
    rows = tokens // blocks
    chunk_rows = 2 * REG // CHUNKS
    spread = width // kv_width * tokens
    far = max(len(stage) for stage in stage_list(devices)) * rows + REG
    dma = pltpu.SemaphoreType.DMA
    pinned = functools.partial(pltpu.with_memory_space_constraint, memory_space=pltpu.HBM)
    anywhere = pl.BlockSpec(memory_space=pltpu.HBM)
    out = pl.pallas_call(
        functools.partial(kernel, devices),
        out_shape=jax.ShapeDtypeStruct((tokens, width), bf),
        in_specs=[anywhere] * 7,
        out_specs=pl.BlockSpec(memory_space=pl.ANY),
        scratch_shapes=[
            pltpu.SMEM((blocks, slots), jnp.int32),
            pltpu.SMEM((blocks,), jnp.int32),
            pltpu.SMEM((blocks,), jnp.int32),
            pltpu.SMEM((1,), jnp.int32),
            pltpu.VMEM((tokens, width), bf),
            pltpu.VMEM((blocks, rows, kv_width), bf),
            pltpu.VMEM((blocks, rows, kv_width), bf),
            pltpu.VMEM((blocks, KEY_VALUE_HEADS, HEAD_SIZE + SUMS, rows), bf),
            pltpu.VMEM((8, 128), jnp.int32),
            pltpu.VMEM((devices, 8, 128), jnp.int32),
            pltpu.VMEM((CHUNKS, chunk_rows, kv_width), bf),
            pltpu.VMEM((devices, chunk_rows, kv_width), bf),
            pltpu.VMEM((chunk_rows, kv_width), bf),
            pltpu.VMEM((devices, chunk_rows, kv_width), bf),
            pltpu.VMEM((devices, KEY_VALUE_HEADS, 2 * rows, HEAD_SIZE), bf),
            pltpu.VMEM((devices, KEY_VALUE_HEADS, 2 * rows, HEAD_SIZE), bf),
            pltpu.VMEM((KEY_VALUE_HEADS, HEAD_SIZE + 8, spread), f32),
            pltpu.VMEM((KEY_VALUE_HEADS, 8, spread), f32),
            pltpu.VMEM((devices, 8, spread), f32),
            pltpu.VMEM((blocks, rows, rows), f32),
            pltpu.VMEM((far, 2 * HEAD_SIZE), bf),
            pltpu.VMEM((HEAD_SIZE + SUMS, far), bf),
            pltpu.VMEM((far, UNITS * rows), f32),
            pltpu.VMEM((far, UNITS * rows), f32),
            pltpu.VMEM((8, UNITS * rows), f32),
            pltpu.VMEM((8, UNITS * rows), f32),
            pltpu.VMEM((max(1, len(late_peers(devices))) * rows, spread), bf),
            pltpu.VMEM((8, spread), f32),
            pltpu.VMEM((tokens, width), bf),
            dma((1,)),
            dma((4,)),
            dma((2,)),
            dma((blocks,)),
            dma((5,)),
            dma((devices - 1,)),
            dma((3,)),
            dma((len(stage_list(devices)) + (1 if late_peers(devices) else 0), KEY_VALUE_HEADS)),
        ],
        compiler_params=pltpu.CompilerParams(
            collective_id=0, has_side_effects=True, vmem_limit_bytes=42 * 1024 * 1024 + devices * kv_width * rows * 4
        ),
    )(
        pinned(block_lists[0]),
        pinned(list_counts[0]),
        pinned(image_blocks[0]),
        reg_owner,
        pinned(queries[0]),
        pinned(keys.reshape(blocks, rows, kv_width)),
        pinned(values.reshape(blocks, rows, kv_width)),
    )
    return out[None]


def solution(mesh):
    placed = (
        P("samp", "seq", None),
        P("samp", "seq", None),
        P("samp", "seq", None),
        P("samp"),
        P("samp", "seq", None),
        P("samp", "seq"),
        P("samp", "seq"),
    )
    return jax.shard_map(
        per_device, mesh=mesh, in_specs=placed, out_specs=P("samp", "seq", None), check_vma=False
    )
```

```python
import functools
import math

import jax
import jax.numpy as jnp
from jax import lax
from jax.experimental import pallas as pl
from jax.experimental.pallas import tpu as pltpu
from jax.sharding import PartitionSpec as P

KEY_VALUE_HEADS = 4
HEAD_SIZE = 128
REG = 64
CHUNKS = 8
SUMS = 16
UNITS = 4

hidden = -1e30
score_gain = math.log2(math.e) / math.sqrt(HEAD_SIZE)
bf = jnp.bfloat16
f32 = jnp.float32


def stage_list(devices):
    if devices == 8:
        return [(1, 2, 4, 3, 5), (6, 7)]
    rest = list(range(1, devices))
    return [tuple(rest[i : i + 7]) for i in range(0, len(rest), 7)]


def late_peers(devices):
    return stage_list(devices)[-1] if devices == 8 else ()


def part_of(entry, blocks):
    if blocks & (blocks - 1):
        return lax.div(entry, blocks), lax.rem(entry, blocks)
    return lax.shift_right_logical(entry, blocks.bit_length() - 1), lax.bitwise_and(entry, blocks - 1)


def split(keys):
    scaled = keys.astype(f32) * score_gain
    high = scaled.astype(bf)
    low = (scaled - high.astype(f32)).astype(bf)
    return high, low


def kernel(
    devices,
    lists_hbm,
    counts_hbm,
    image_hbm,
    owner_hbm,
    q_hbm,
    k_hbm,
    v_hbm,
    out_ref,
    lists_ref,
    counts_ref,
    image_ref,
    owner_ref,
    q_all,
    k_all,
    v_all,
    vt_own,
    need_out,
    need_in,
    chunk_out,
    chunk_in,
    reg_out,
    reg_in,
    x_out,
    x_in,
    acc,
    top,
    shown,
    own_mask,
    kk,
    vt,
    s_a,
    s_b,
    m_a,
    m_b,
    held,
    held_top,
    out_all,
    out_sem,
    small_sem,
    local_sem,
    q_sem,
    send_sem,
    recv_need,
    recv_sem,
    recv_x,
):
    me = lax.axis_index("seq")
    blocks, slots = lists_ref.shape
    rows = k_hbm.shape[1]
    heads = q_hbm.shape[1] // HEAD_SIZE
    group = heads // KEY_VALUE_HEADS
    chunk_rows = 2 * REG // CHUNKS
    peers = range(1, devices)
    wide = UNITS * rows
    steps = blocks * group // UNITS
    late = late_peers(devices)
    stages = stage_list(devices)

    def peer(k):
        return me ^ k

    small = [
        pltpu.make_async_copy(lists_hbm, lists_ref, small_sem.at[0]),
        pltpu.make_async_copy(counts_hbm, counts_ref, small_sem.at[1]),
        pltpu.make_async_copy(image_hbm, image_ref, small_sem.at[2]),
        pltpu.make_async_copy(owner_hbm, owner_ref, small_sem.at[3]),
    ]
    for copy in small:
        copy.start()
    k_copy = pltpu.make_async_copy(k_hbm, k_all, local_sem.at[0])
    v_copy = pltpu.make_async_copy(v_hbm, v_all, local_sem.at[1])
    k_copy.start()
    v_copy.start()
    barrier = pltpu.get_barrier_semaphore()
    for k in peers:
        pl.semaphore_signal(barrier, inc=1, device_id={"seq": peer(k)})

    def q_copy(b):
        span = pl.ds(pl.multiple_of(b * rows, rows), rows)
        return pltpu.make_async_copy(q_hbm.at[span], q_all.at[span], q_sem.at[b])

    for b in range(blocks):
        q_copy(b).start()

    for copy in small:
        copy.wait()
    lane = lax.broadcasted_iota(jnp.int32, (8, 128), 1)
    wanted = jnp.zeros((8, 128), jnp.int32)
    sources = []
    for b in range(blocks):
        count = counts_ref[b]
        sources.append([])
        for t in range(slots):
            source, local = part_of(lists_ref[b, t], blocks)
            source = jnp.where(t < count, source, -1)
            sources[b].append(source)
            wanted = jnp.where(lane == source, local, wanted)
    need_out[...] = wanted
    k_copy.wait()
    v_copy.wait()
    for c in range(CHUNKS):
        whole = k_all if c < CHUNKS // 2 else v_all
        start = (c % (CHUNKS // 2)) * chunk_rows
        chunk_out[c] = whole[0, start : start + chunk_rows]
    pl.semaphore_wait(barrier, devices - 1)

    def need_copy(k):
        return pltpu.make_async_remote_copy(
            need_out, need_in.at[k], send_sem.at[0], recv_need.at[k - 1], device_id={"seq": peer(k)}
        )

    def chunk_copy(k):
        return pltpu.make_async_remote_copy(
            chunk_out.at[lax.rem(peer(k), CHUNKS)],
            chunk_in.at[me],
            send_sem.at[1],
            recv_sem.at[0],
            device_id={"seq": peer(k)},
        )

    alike = range(2, devices, 2)

    def reg_copy(k):
        return pltpu.make_async_remote_copy(
            reg_out, reg_in.at[me], send_sem.at[2], recv_sem.at[1], device_id={"seq": peer(k)}
        )

    def pass_copy(k):
        return pltpu.make_async_remote_copy(
            reg_in.at[peer(k)], reg_in.at[peer(k)], send_sem.at[3], recv_sem.at[2], device_id={"seq": peer(1)}
        )

    def x_copy(k, g, part):
        span = pl.ds(part * rows, rows if k in late else 2 * rows)
        n = [k in stage for stage in stages].index(True) + part
        return pltpu.make_async_remote_copy(
            x_out.at[k, g, span], x_in.at[k, g, span], send_sem.at[4], recv_x.at[n, g], device_id={"seq": peer(k)}
        )

    def total(ref, kind, received):
        return pltpu.make_async_remote_copy(ref, ref, send_sem.at[kind], received, device_id={"seq": peer(1)})

    def arrive(stage, g, part):
        span = pl.ds(part * rows, rows if stage == late else 2 * rows)
        ref = x_in.at[pl.ds(min(stage), len(stage)), g, span]
        total(ref, 4, recv_x.at[stages.index(stage) + part, g]).wait_recv()

    order = list(reversed(peers))
    for k in order:
        need_copy(k).start()
    for k in order:
        chunk_copy(k).start()
    chunk_in[me] = chunk_out[lax.rem(me, CHUNKS)]

    for b in range(blocks):
        for g in range(KEY_VALUE_HEADS):
            column = slice(g * HEAD_SIZE, (g + 1) * HEAD_SIZE)
            vt_own[b, g, :HEAD_SIZE] = v_all[b, :, column].T
            vt_own[b, g, HEAD_SIZE:] = jnp.ones((SUMS, rows), bf)

    picks = {}

    def fill(k, g):
        columns = pl.ds(g * HEAD_SIZE, HEAD_SIZE)
        x_out[k, g, :rows] = k_all[picks[k], :, columns]
        x_out[k, g, rows:] = vt_own[picks[k], g, :HEAD_SIZE]

    def answer(k):
        need_copy(k).wait_recv()
        row = need_in[k]
        picks[k] = jnp.sum(jnp.where(lane[:1] == me, row[:1], 0))
        if k in stages[0]:
            fill(k, 0)
            x_copy(k, 0, 0).start()

    everyone = [k for stage in stages for k in stage]
    for k in everyone[:3]:
        answer(k)
    total(chunk_in.at[pl.ds(0, devices - 1)], 1, recv_sem.at[0]).wait_recv()
    mine = chunk_in[owner_ref[0]]
    reg_out[...] = mine
    reg_in[me] = mine
    for k in reversed(alike):
        reg_copy(k).start()
    pass_copy(0).start()
    for k in everyone[3:]:
        answer(k)

    def send(chosen, g, turned=False):
        for stage in chosen:
            for k in sorted(stage, key=lambda k: -(k % 2)) if turned else stage:
                fill(k, g)
                x_copy(k, g, 0).start()
        for k in late:
            if late in chosen:
                x_copy(k, g, 1).start()

    early, final = stages[:-1], stages[-1:]

    for k in peers:
        source = peer(k)
        for b in range(blocks):
            seen = functools.reduce(jnp.logical_or, [found == source for found in sources[b]])
            value = jnp.where(seen, 0.0, hidden)
            shown[k, :, b * group * rows : (b + 1) * group * rows] = jnp.full((8, group * rows), value)

    key_side = lax.broadcasted_iota(jnp.int32, (rows, rows), 0)
    row_side = lax.broadcasted_iota(jnp.int32, (rows, rows), 1)
    for b in range(blocks):
        shut = jnp.where(image_ref[b] == 1, 0.0, hidden)
        own_mask[b] = jnp.where(key_side <= row_side, 0.0, shut)
    vt[HEAD_SIZE:] = jnp.ones((SUMS, vt.shape[1]), bf)

    nt = (((1,), (1,)), ((), ()))

    def own_step(b, carry):
        @pl.when(b == 1)
        def _():
            send(early[1:], 0)
            send(early, 1, True)

        @pl.when(b == blocks - 1)
        def _():
            total(reg_in.at[pl.ds(0, len(alike))], 2, recv_sem.at[1]).wait_recv()
            for k in alike:
                pass_copy(k).start()

        q_copy(b).wait()
        row_span = pl.ds(pl.multiple_of(b * rows, rows), rows)
        place = pl.ds(pl.multiple_of(b * group * rows, rows), group * rows)
        mask = jnp.concatenate([own_mask[b]] * group, axis=1)

        def scored(g):
            own_keys = k_all[b, :, g * HEAD_SIZE : (g + 1) * HEAD_SIZE]
            query = jnp.concatenate(
                [
                    q_all[row_span, (g * group + h) * HEAD_SIZE : (g * group + h + 1) * HEAD_SIZE]
                    for h in range(group)
                ],
                axis=0,
            )
            return lax.dot_general(own_keys, query, nt, preferred_element_type=f32) * score_gain + mask

        ahead = scored(0)
        for g in range(KEY_VALUE_HEADS):
            scores = ahead
            if g + 1 < KEY_VALUE_HEADS:
                ahead = scored(g + 1)
            best = jnp.max(scores, axis=0, keepdims=True)
            weights = jnp.exp2(scores - best).astype(bf)
            product = jnp.dot(vt_own[b, g], weights, preferred_element_type=f32)
            acc[g, :, place] = product[: HEAD_SIZE + 8]
            top[g, :, place] = jnp.broadcast_to(best, (8, group * rows))
        return carry

    lax.fori_loop(0, blocks, own_step, 0)
    total(reg_in.at[pl.ds(0, devices // 2)], 3, recv_sem.at[2]).wait_recv()

    half = CHUNKS // 2

    def far_stage(g, stage, first, last):
        size_all = len(stage) * rows + (REG if first else 0)
        apart = stage == late
        arrive(stage, g, 0)
        if first:

            @pl.when(g < KEY_VALUE_HEADS - 1)
            def _():
                send(final, g)

            @pl.when(g < KEY_VALUE_HEADS - 2)
            def _():
                send(early, g + 2)

            @pl.when(g == KEY_VALUE_HEADS - 2)
            def _():
                send(final, KEY_VALUE_HEADS - 1)

        for n, k in enumerate(stage):
            high, low = split(x_in[k, g, :rows])
            kk[n * rows : (n + 1) * rows, :HEAD_SIZE] = high
            kk[n * rows : (n + 1) * rows, HEAD_SIZE:] = low

        def load_values():
            for n, k in enumerate(stage):
                vt[:HEAD_SIZE, n * rows : (n + 1) * rows] = x_in[k, g, rows:]

        if not apart:
            load_values()
        if first:
            column = pl.ds(pl.multiple_of(g * HEAD_SIZE, HEAD_SIZE), HEAD_SIZE)
            begin = len(stage) * rows
            high, low = split(reg_in[pl.ds(0, half), :, column].reshape(REG, HEAD_SIZE))
            kk[begin : begin + REG, :HEAD_SIZE] = high
            kk[begin : begin + REG, HEAD_SIZE:] = low
            vt[:HEAD_SIZE, begin : begin + REG] = reg_in[pl.ds(half, half), :, column].reshape(REG, HEAD_SIZE).T

        pieces = [(n * rows, rows, k) for n, k in enumerate(stage)]
        if first:
            pieces.append((len(stage) * rows, REG, None))

        def unit(j, n):
            u = j * UNITS + n
            b, h = u // group, u % group
            column = pl.ds(pl.multiple_of((g * group + h) * HEAD_SIZE, HEAD_SIZE), HEAD_SIZE)
            return pl.ds(b * rows, rows), column

        def place_of(j):
            return pl.ds(j * wide, wide)

        def score(j, s_ref, m_ref):
            place = place_of(j)
            query = jnp.concatenate([q_all[unit(j, n)] for n in range(UNITS)], axis=0)
            query = jnp.concatenate([query, query], axis=1)
            scores = lax.dot_general(kk[:size_all], query, nt, preferred_element_type=f32)
            s_ref[:size_all] = scores
            best = top[g, :, place]
            for begin, size, k in pieces:
                block = jnp.max(scores[begin : begin + size].reshape(size // 8, 8, wide), axis=0)
                best = jnp.maximum(best, block if k is None else block + shown[k, :, place])
            m_ref[...] = jnp.broadcast_to(jnp.max(best, axis=0, keepdims=True), (8, wide))

        def weigh(j, s_ref, best, chosen):
            parts = []
            for begin, size, k in chosen:
                shift = -best if k is None else shown[k, :, place_of(j)] - best
                block = s_ref[begin : begin + size].reshape(size // 8, 8, wide)
                parts.append(jnp.exp2(block + shift[None]).reshape(size, wide).astype(bf))
            return jnp.concatenate(parts, axis=0)

        def finish(j, product, best):
            place = place_of(j)
            scale = jnp.exp2(top[g, :, place] - best)
            product = product[: HEAD_SIZE + 8].reshape(HEAD_SIZE // 8 + 1, 8, wide)
            product = product + acc[g, :, place].reshape(HEAD_SIZE // 8 + 1, 8, wide) * scale[None]
            if last:
                share = 1.0 / product[HEAD_SIZE // 8]
                merged = (product[: HEAD_SIZE // 8] * share[None]).reshape(HEAD_SIZE, wide).astype(bf)
                for n in range(UNITS):
                    out_all[unit(j, n)] = merged[:, n * rows : (n + 1) * rows].T
            else:
                acc[g, :, place] = product.reshape(HEAD_SIZE + 8, wide)
                top[g, :, place] = best

        def merge(j, s_ref, m_ref):
            best = m_ref[...]
            product = None
            for c in range(0, len(pieces), 2):
                begin = pieces[c][0]
                weights = weigh(j, s_ref, best, pieces[c : c + 2])
                more = jnp.dot(vt[:, begin : begin + weights.shape[0]], weights, preferred_element_type=f32)
                product = more if product is None else product + more
            finish(j, product, best)

        def keep(j, s_ref, m_ref):
            best = m_ref[...]
            held[:, place_of(j)] = weigh(j, s_ref, best, pieces)
            held_top[:, place_of(j)] = best

        score(0, s_a, m_a)
        buffers = ((s_a, m_a), (s_b, m_b))
        for j in range(steps):
            if j + 1 < steps:
                score(j + 1, *buffers[(j + 1) % 2])
            (keep if apart else merge)(j, *buffers[j % 2])
        if apart:
            arrive(stage, g, 1)
            load_values()
            for j in range(steps):
                product = jnp.dot(vt[:, :size_all], held[:, place_of(j)], preferred_element_type=f32)
                finish(j, product, held_top[:, place_of(j)])

    def out_copy(g):
        span = pl.ds(pl.multiple_of(g * group * HEAD_SIZE, HEAD_SIZE), group * HEAD_SIZE)
        return pltpu.make_async_copy(out_all.at[:, span], out_ref.at[:, span], out_sem.at[0])

    def near_part(g):
        for stage in early:
            far_stage(g, stage, stage == stages[0], False)

    def far_part(g):
        far_stage(g, final[0], False, True)
        out_copy(g).start()

    def far_group(g, carry):
        near_part(g)
        far_part(g - 1)
        return carry

    near_part(jnp.int32(0))
    lax.fori_loop(1, KEY_VALUE_HEADS, far_group, 0)
    far_part(KEY_VALUE_HEADS - 1)

    pltpu.make_async_copy(out_all, out_ref, out_sem.at[0]).wait()
    total(need_in.at[pl.ds(0, devices - 1)], 0, recv_sem.at[0]).wait_send()
    total(chunk_in.at[pl.ds(0, devices - 1)], 1, recv_sem.at[0]).wait_send()
    total(reg_in.at[pl.ds(0, len(alike))], 2, recv_sem.at[1]).wait_send()
    total(reg_in.at[pl.ds(0, devices // 2)], 3, recv_sem.at[2]).wait_send()
    total(x_out.at[pl.ds(1, devices - 1)], 4, recv_sem.at[0]).wait_send()


def per_device(queries, keys, values, reg_owner, block_lists, list_counts, image_blocks):
    devices = lax.axis_size("seq")
    tokens, width = queries.shape[1:]
    kv_width = keys.shape[2]
    blocks, slots = block_lists.shape[1:]
    rows = tokens // blocks
    chunk_rows = 2 * REG // CHUNKS
    spread = width // kv_width * tokens
    far = max(len(stage) for stage in stage_list(devices)) * rows + REG
    dma = pltpu.SemaphoreType.DMA
    pinned = functools.partial(pltpu.with_memory_space_constraint, memory_space=pltpu.HBM)
    anywhere = pl.BlockSpec(memory_space=pltpu.HBM)
    out = pl.pallas_call(
        functools.partial(kernel, devices),
        out_shape=jax.ShapeDtypeStruct((tokens, width), bf),
        in_specs=[anywhere] * 7,
        out_specs=pl.BlockSpec(memory_space=pl.ANY),
        scratch_shapes=[
            pltpu.SMEM((blocks, slots), jnp.int32),
            pltpu.SMEM((blocks,), jnp.int32),
            pltpu.SMEM((blocks,), jnp.int32),
            pltpu.SMEM((1,), jnp.int32),
            pltpu.VMEM((tokens, width), bf),
            pltpu.VMEM((blocks, rows, kv_width), bf),
            pltpu.VMEM((blocks, rows, kv_width), bf),
            pltpu.VMEM((blocks, KEY_VALUE_HEADS, HEAD_SIZE + SUMS, rows), bf),
            pltpu.VMEM((8, 128), jnp.int32),
            pltpu.VMEM((devices, 8, 128), jnp.int32),
            pltpu.VMEM((CHUNKS, chunk_rows, kv_width), bf),
            pltpu.VMEM((devices, chunk_rows, kv_width), bf),
            pltpu.VMEM((chunk_rows, kv_width), bf),
            pltpu.VMEM((devices, chunk_rows, kv_width), bf),
            pltpu.VMEM((devices, KEY_VALUE_HEADS, 2 * rows, HEAD_SIZE), bf),
            pltpu.VMEM((devices, KEY_VALUE_HEADS, 2 * rows, HEAD_SIZE), bf),
            pltpu.VMEM((KEY_VALUE_HEADS, HEAD_SIZE + 8, spread), f32),
            pltpu.VMEM((KEY_VALUE_HEADS, 8, spread), f32),
            pltpu.VMEM((devices, 8, spread), f32),
            pltpu.VMEM((blocks, rows, rows), f32),
            pltpu.VMEM((far, 2 * HEAD_SIZE), bf),
            pltpu.VMEM((HEAD_SIZE + SUMS, far), bf),
            pltpu.VMEM((far, UNITS * rows), f32),
            pltpu.VMEM((far, UNITS * rows), f32),
            pltpu.VMEM((8, UNITS * rows), f32),
            pltpu.VMEM((8, UNITS * rows), f32),
            pltpu.VMEM((max(1, len(late_peers(devices))) * rows, spread), bf),
            pltpu.VMEM((8, spread), f32),
            pltpu.VMEM((tokens, width), bf),
            dma((1,)),
            dma((4,)),
            dma((2,)),
            dma((blocks,)),
            dma((5,)),
            dma((devices - 1,)),
            dma((3,)),
            dma((len(stage_list(devices)) + (1 if late_peers(devices) else 0), KEY_VALUE_HEADS)),
        ],
        compiler_params=pltpu.CompilerParams(
            collective_id=0, has_side_effects=True, vmem_limit_bytes=42 * 1024 * 1024 + devices * kv_width * rows * 4
        ),
    )(
        pinned(block_lists[0]),
        pinned(list_counts[0]),
        pinned(image_blocks[0]),
        reg_owner,
        pinned(queries[0]),
        pinned(keys.reshape(blocks, rows, kv_width)),
        pinned(values.reshape(blocks, rows, kv_width)),
    )
    return out[None]


def solution(mesh):
    placed = (
        P("samp", "seq", None),
        P("samp", "seq", None),
        P("samp", "seq", None),
        P("samp"),
        P("samp", "seq", None),
        P("samp", "seq"),
        P("samp", "seq"),
    )
    return jax.shard_map(
        per_device, mesh=mesh, in_specs=placed, out_specs=P("samp", "seq", None), check_vma=False
    )
```

```python
import functools
import math

import jax
import jax.numpy as jnp
from jax import lax
from jax.experimental import pallas as pl
from jax.experimental.pallas import tpu as pltpu
from jax.sharding import PartitionSpec as P

KEY_VALUE_HEADS = 4
HEAD_SIZE = 128
REG = 64
CHUNKS = 8
SUMS = 16
UNITS = 4

hidden = -1e30
score_gain = math.log2(math.e) / math.sqrt(HEAD_SIZE)
bf = jnp.bfloat16
f32 = jnp.float32


def stage_list(devices):
    if devices == 8:
        return [(1, 2, 4, 3, 5), (6, 7)]
    rest = list(range(1, devices))
    return [tuple(rest[i : i + 7]) for i in range(0, len(rest), 7)]


def late_peers(devices):
    return stage_list(devices)[-1] if devices == 8 else ()


def part_of(entry, blocks):
    if blocks & (blocks - 1):
        return lax.div(entry, blocks), lax.rem(entry, blocks)
    return lax.shift_right_logical(entry, blocks.bit_length() - 1), lax.bitwise_and(entry, blocks - 1)


def split(keys):
    scaled = keys.astype(f32) * score_gain
    high = scaled.astype(bf)
    low = (scaled - high.astype(f32)).astype(bf)
    return high, low


def kernel(
    devices,
    lists_hbm,
    counts_hbm,
    image_hbm,
    owner_hbm,
    q_hbm,
    k_hbm,
    v_hbm,
    out_ref,
    lists_ref,
    counts_ref,
    image_ref,
    owner_ref,
    q_all,
    k_all,
    v_all,
    vt_own,
    need_out,
    need_in,
    chunk_out,
    chunk_in,
    reg_out,
    reg_in,
    x_out,
    x_in,
    acc,
    top,
    shown,
    own_mask,
    kk,
    vt,
    s_a,
    s_b,
    m_a,
    m_b,
    held,
    held_top,
    out_all,
    out_sem,
    small_sem,
    local_sem,
    q_sem,
    send_sem,
    recv_need,
    recv_sem,
    recv_x,
):
    me = lax.axis_index("seq")
    blocks, slots = lists_ref.shape
    rows = k_hbm.shape[1]
    heads = q_hbm.shape[1] // HEAD_SIZE
    group = heads // KEY_VALUE_HEADS
    chunk_rows = 2 * REG // CHUNKS
    peers = range(1, devices)
    wide = UNITS * rows
    steps = blocks * group // UNITS
    late = late_peers(devices)
    stages = stage_list(devices)

    def peer(k):
        return me ^ k

    small = [
        pltpu.make_async_copy(lists_hbm, lists_ref, small_sem.at[0]),
        pltpu.make_async_copy(counts_hbm, counts_ref, small_sem.at[1]),
        pltpu.make_async_copy(image_hbm, image_ref, small_sem.at[2]),
        pltpu.make_async_copy(owner_hbm, owner_ref, small_sem.at[3]),
    ]
    for copy in small:
        copy.start()
    k_copy = pltpu.make_async_copy(k_hbm, k_all, local_sem.at[0])
    v_copy = pltpu.make_async_copy(v_hbm, v_all, local_sem.at[1])
    k_copy.start()
    v_copy.start()
    barrier = pltpu.get_barrier_semaphore()
    for k in peers:
        pl.semaphore_signal(barrier, inc=1, device_id={"seq": peer(k)})

    def q_copy(b):
        span = pl.ds(pl.multiple_of(b * rows, rows), rows)
        return pltpu.make_async_copy(q_hbm.at[span], q_all.at[span], q_sem.at[b])

    for b in range(blocks):
        q_copy(b).start()

    for copy in small:
        copy.wait()
    lane = lax.broadcasted_iota(jnp.int32, (8, 128), 1)
    wanted = jnp.zeros((8, 128), jnp.int32)
    sources = []
    for b in range(blocks):
        count = counts_ref[b]
        sources.append([])
        for t in range(slots):
            source, local = part_of(lists_ref[b, t], blocks)
            source = jnp.where(t < count, source, -1)
            sources[b].append(source)
            wanted = jnp.where(lane == source, local, wanted)
    need_out[...] = wanted
    k_copy.wait()
    v_copy.wait()
    for c in range(CHUNKS):
        whole = k_all if c < CHUNKS // 2 else v_all
        start = (c % (CHUNKS // 2)) * chunk_rows
        chunk_out[c] = whole[0, start : start + chunk_rows]
    pl.semaphore_wait(barrier, devices - 1)

    def need_copy(k):
        return pltpu.make_async_remote_copy(
            need_out, need_in.at[k], send_sem.at[0], recv_need.at[k - 1], device_id={"seq": peer(k)}
        )

    def chunk_copy(k):
        return pltpu.make_async_remote_copy(
            chunk_out.at[lax.rem(peer(k), CHUNKS)],
            chunk_in.at[me],
            send_sem.at[1],
            recv_sem.at[0],
            device_id={"seq": peer(k)},
        )

    alike = range(2, devices, 2)

    def reg_copy(k):
        return pltpu.make_async_remote_copy(
            reg_out, reg_in.at[me], send_sem.at[2], recv_sem.at[1], device_id={"seq": peer(k)}
        )

    def pass_copy(k):
        return pltpu.make_async_remote_copy(
            reg_in.at[peer(k)], reg_in.at[peer(k)], send_sem.at[3], recv_sem.at[2], device_id={"seq": peer(1)}
        )

    def x_copy(k, g, part):
        span = pl.ds(part * rows, rows if k in late else 2 * rows)
        n = [k in stage for stage in stages].index(True) + part
        return pltpu.make_async_remote_copy(
            x_out.at[k, g, span], x_in.at[k, g, span], send_sem.at[4], recv_x.at[n, g], device_id={"seq": peer(k)}
        )

    def total(ref, kind, received):
        return pltpu.make_async_remote_copy(ref, ref, send_sem.at[kind], received, device_id={"seq": peer(1)})

    def arrive(stage, g, part):
        span = pl.ds(part * rows, rows if stage == late else 2 * rows)
        ref = x_in.at[pl.ds(min(stage), len(stage)), g, span]
        total(ref, 4, recv_x.at[stages.index(stage) + part, g]).wait_recv()

    order = list(reversed(peers))
    for k in order:
        need_copy(k).start()
    for k in order:
        chunk_copy(k).start()
    chunk_in[me] = chunk_out[lax.rem(me, CHUNKS)]

    for b in range(blocks):
        for g in range(KEY_VALUE_HEADS):
            column = slice(g * HEAD_SIZE, (g + 1) * HEAD_SIZE)
            vt_own[b, g, :HEAD_SIZE] = v_all[b, :, column].T
            vt_own[b, g, HEAD_SIZE:] = jnp.ones((SUMS, rows), bf)

    key_side = lax.broadcasted_iota(jnp.int32, (rows, rows), 0)
    row_side = lax.broadcasted_iota(jnp.int32, (rows, rows), 1)
    for b in range(blocks):
        shut = jnp.where(image_ref[b] == 1, 0.0, hidden)
        own_mask[b] = jnp.where(key_side <= row_side, 0.0, shut)
    nt = (((1,), (1,)), ((), ()))

    def own_block(b, carry):
        q_copy(b).wait()
        row_span = pl.ds(pl.multiple_of(b * rows, rows), rows)
        place = pl.ds(pl.multiple_of(b * group * rows, rows), group * rows)
        mask = jnp.concatenate([own_mask[b]] * group, axis=1)

        def scored(g):
            own_keys = k_all[b, :, g * HEAD_SIZE : (g + 1) * HEAD_SIZE]
            query = jnp.concatenate(
                [
                    q_all[row_span, (g * group + h) * HEAD_SIZE : (g * group + h + 1) * HEAD_SIZE]
                    for h in range(group)
                ],
                axis=0,
            )
            return lax.dot_general(own_keys, query, nt, preferred_element_type=f32) * score_gain + mask

        ahead = scored(0)
        for g in range(KEY_VALUE_HEADS):
            scores = ahead
            if g + 1 < KEY_VALUE_HEADS:
                ahead = scored(g + 1)
            best = jnp.max(scores, axis=0, keepdims=True)
            weights = jnp.exp2(scores - best).astype(bf)
            product = jnp.dot(vt_own[b, g], weights, preferred_element_type=f32)
            acc[g, :, place] = product[: HEAD_SIZE + 8]
            top[g, :, place] = jnp.broadcast_to(best, (8, group * rows))
        return carry

    lax.fori_loop(0, 1, own_block, 0)

    picks = {}

    def fill(k, g):
        columns = pl.ds(g * HEAD_SIZE, HEAD_SIZE)
        x_out[k, g, :rows] = k_all[picks[k], :, columns]
        x_out[k, g, rows:] = vt_own[picks[k], g, :HEAD_SIZE]

    def answer(k):
        need_copy(k).wait_recv()
        row = need_in[k]
        picks[k] = jnp.sum(jnp.where(lane[:1] == me, row[:1], 0))
        if k in stages[0]:
            fill(k, 0)
            x_copy(k, 0, 0).start()

    everyone = [k for stage in stages for k in stage]
    for k in everyone[:3]:
        answer(k)
    total(chunk_in.at[pl.ds(0, devices - 1)], 1, recv_sem.at[0]).wait_recv()
    mine = chunk_in[owner_ref[0]]
    reg_out[...] = mine
    reg_in[me] = mine
    for k in reversed(alike):
        reg_copy(k).start()
    pass_copy(0).start()
    for k in everyone[3:]:
        answer(k)

    def send(chosen, g, turned=False):
        for stage in chosen:
            for k in sorted(stage, key=lambda k: -(k % 2)) if turned else stage:
                fill(k, g)
                x_copy(k, g, 0).start()
        for k in late:
            if late in chosen:
                x_copy(k, g, 1).start()

    early, final = stages[:-1], stages[-1:]

    for k in peers:
        source = peer(k)
        for b in range(blocks):
            seen = functools.reduce(jnp.logical_or, [found == source for found in sources[b]])
            value = jnp.where(seen, 0.0, hidden)
            shown[k, :, b * group * rows : (b + 1) * group * rows] = jnp.full((8, group * rows), value)

    vt[HEAD_SIZE:] = jnp.ones((SUMS, vt.shape[1]), bf)


    def own_step(b, carry):
        @pl.when(b == 1)
        def _():
            send(early[1:], 0)
            send(early, 1, True)

        @pl.when(b == blocks - 1)
        def _():
            total(reg_in.at[pl.ds(0, len(alike))], 2, recv_sem.at[1]).wait_recv()
            for k in alike:
                pass_copy(k).start()

        return own_block(b, carry)

    lax.fori_loop(1, blocks, own_step, 0)
    total(reg_in.at[pl.ds(0, devices // 2)], 3, recv_sem.at[2]).wait_recv()

    half = CHUNKS // 2

    def far_stage(g, stage, first, last):
        size_all = len(stage) * rows + (REG if first else 0)
        apart = stage == late
        arrive(stage, g, 0)
        if first:

            @pl.when(g < KEY_VALUE_HEADS - 1)
            def _():
                send(final, g)

            @pl.when(g < KEY_VALUE_HEADS - 2)
            def _():
                send(early, g + 2)

            @pl.when(g == KEY_VALUE_HEADS - 2)
            def _():
                send(final, KEY_VALUE_HEADS - 1)

        for n, k in enumerate(stage):
            high, low = split(x_in[k, g, :rows])
            kk[n * rows : (n + 1) * rows, :HEAD_SIZE] = high
            kk[n * rows : (n + 1) * rows, HEAD_SIZE:] = low

        def load_values():
            for n, k in enumerate(stage):
                vt[:HEAD_SIZE, n * rows : (n + 1) * rows] = x_in[k, g, rows:]

        if not apart:
            load_values()
        if first:
            column = pl.ds(pl.multiple_of(g * HEAD_SIZE, HEAD_SIZE), HEAD_SIZE)
            begin = len(stage) * rows
            high, low = split(reg_in[pl.ds(0, half), :, column].reshape(REG, HEAD_SIZE))
            kk[begin : begin + REG, :HEAD_SIZE] = high
            kk[begin : begin + REG, HEAD_SIZE:] = low
            vt[:HEAD_SIZE, begin : begin + REG] = reg_in[pl.ds(half, half), :, column].reshape(REG, HEAD_SIZE).T

        pieces = [(n * rows, rows, k) for n, k in enumerate(stage)]
        if first:
            pieces.append((len(stage) * rows, REG, None))

        def unit(j, n):
            u = j * UNITS + n
            b, h = u // group, u % group
            column = pl.ds(pl.multiple_of((g * group + h) * HEAD_SIZE, HEAD_SIZE), HEAD_SIZE)
            return pl.ds(b * rows, rows), column

        def place_of(j):
            return pl.ds(j * wide, wide)

        def score(j, s_ref, m_ref):
            place = place_of(j)
            query = jnp.concatenate([q_all[unit(j, n)] for n in range(UNITS)], axis=0)
            query = jnp.concatenate([query, query], axis=1)
            scores = lax.dot_general(kk[:size_all], query, nt, preferred_element_type=f32)
            s_ref[:size_all] = scores
            best = top[g, :, place]
            for begin, size, k in pieces:
                block = jnp.max(scores[begin : begin + size].reshape(size // 8, 8, wide), axis=0)
                best = jnp.maximum(best, block if k is None else block + shown[k, :, place])
            m_ref[...] = jnp.broadcast_to(jnp.max(best, axis=0, keepdims=True), (8, wide))

        def weigh(j, s_ref, best, chosen):
            parts = []
            for begin, size, k in chosen:
                shift = -best if k is None else shown[k, :, place_of(j)] - best
                block = s_ref[begin : begin + size].reshape(size // 8, 8, wide)
                parts.append(jnp.exp2(block + shift[None]).reshape(size, wide).astype(bf))
            return jnp.concatenate(parts, axis=0)

        def finish(j, product, best):
            place = place_of(j)
            scale = jnp.exp2(top[g, :, place] - best)
            product = product[: HEAD_SIZE + 8].reshape(HEAD_SIZE // 8 + 1, 8, wide)
            product = product + acc[g, :, place].reshape(HEAD_SIZE // 8 + 1, 8, wide) * scale[None]
            if last:
                share = 1.0 / product[HEAD_SIZE // 8]
                merged = (product[: HEAD_SIZE // 8] * share[None]).reshape(HEAD_SIZE, wide).astype(bf)
                for n in range(UNITS):
                    out_all[unit(j, n)] = merged[:, n * rows : (n + 1) * rows].T
            else:
                acc[g, :, place] = product.reshape(HEAD_SIZE + 8, wide)
                top[g, :, place] = best

        def merge(j, s_ref, m_ref):
            best = m_ref[...]
            product = None
            for c in range(0, len(pieces), 2):
                begin = pieces[c][0]
                weights = weigh(j, s_ref, best, pieces[c : c + 2])
                more = jnp.dot(vt[:, begin : begin + weights.shape[0]], weights, preferred_element_type=f32)
                product = more if product is None else product + more
            finish(j, product, best)

        def keep(j, s_ref, m_ref):
            best = m_ref[...]
            held[:, place_of(j)] = weigh(j, s_ref, best, pieces)
            held_top[:, place_of(j)] = best

        score(0, s_a, m_a)
        buffers = ((s_a, m_a), (s_b, m_b))
        for j in range(steps):
            if j + 1 < steps:
                score(j + 1, *buffers[(j + 1) % 2])
            (keep if apart else merge)(j, *buffers[j % 2])
        if apart:
            arrive(stage, g, 1)
            load_values()
            for j in range(steps):
                product = jnp.dot(vt[:, :size_all], held[:, place_of(j)], preferred_element_type=f32)
                finish(j, product, held_top[:, place_of(j)])

    def out_copy(g):
        span = pl.ds(pl.multiple_of(g * group * HEAD_SIZE, HEAD_SIZE), group * HEAD_SIZE)
        return pltpu.make_async_copy(out_all.at[:, span], out_ref.at[:, span], out_sem.at[0])

    def near_part(g):
        for stage in early:
            far_stage(g, stage, stage == stages[0], False)

    def far_part(g):
        far_stage(g, final[0], False, True)
        out_copy(g).start()

    def far_group(g, carry):
        near_part(g)
        far_part(g - 1)
        return carry

    near_part(jnp.int32(0))
    lax.fori_loop(1, KEY_VALUE_HEADS, far_group, 0)
    far_part(KEY_VALUE_HEADS - 1)

    pltpu.make_async_copy(out_all, out_ref, out_sem.at[0]).wait()
    total(need_in.at[pl.ds(0, devices - 1)], 0, recv_sem.at[0]).wait_send()
    total(chunk_in.at[pl.ds(0, devices - 1)], 1, recv_sem.at[0]).wait_send()
    total(reg_in.at[pl.ds(0, len(alike))], 2, recv_sem.at[1]).wait_send()
    total(reg_in.at[pl.ds(0, devices // 2)], 3, recv_sem.at[2]).wait_send()
    total(x_out.at[pl.ds(1, devices - 1)], 4, recv_sem.at[0]).wait_send()


def per_device(queries, keys, values, reg_owner, block_lists, list_counts, image_blocks):
    devices = lax.axis_size("seq")
    tokens, width = queries.shape[1:]
    kv_width = keys.shape[2]
    blocks, slots = block_lists.shape[1:]
    rows = tokens // blocks
    chunk_rows = 2 * REG // CHUNKS
    spread = width // kv_width * tokens
    far = max(len(stage) for stage in stage_list(devices)) * rows + REG
    dma = pltpu.SemaphoreType.DMA
    pinned = functools.partial(pltpu.with_memory_space_constraint, memory_space=pltpu.HBM)
    anywhere = pl.BlockSpec(memory_space=pltpu.HBM)
    out = pl.pallas_call(
        functools.partial(kernel, devices),
        out_shape=jax.ShapeDtypeStruct((tokens, width), bf),
        in_specs=[anywhere] * 7,
        out_specs=pl.BlockSpec(memory_space=pl.ANY),
        scratch_shapes=[
            pltpu.SMEM((blocks, slots), jnp.int32),
            pltpu.SMEM((blocks,), jnp.int32),
            pltpu.SMEM((blocks,), jnp.int32),
            pltpu.SMEM((1,), jnp.int32),
            pltpu.VMEM((tokens, width), bf),
            pltpu.VMEM((blocks, rows, kv_width), bf),
            pltpu.VMEM((blocks, rows, kv_width), bf),
            pltpu.VMEM((blocks, KEY_VALUE_HEADS, HEAD_SIZE + SUMS, rows), bf),
            pltpu.VMEM((8, 128), jnp.int32),
            pltpu.VMEM((devices, 8, 128), jnp.int32),
            pltpu.VMEM((CHUNKS, chunk_rows, kv_width), bf),
            pltpu.VMEM((devices, chunk_rows, kv_width), bf),
            pltpu.VMEM((chunk_rows, kv_width), bf),
            pltpu.VMEM((devices, chunk_rows, kv_width), bf),
            pltpu.VMEM((devices, KEY_VALUE_HEADS, 2 * rows, HEAD_SIZE), bf),
            pltpu.VMEM((devices, KEY_VALUE_HEADS, 2 * rows, HEAD_SIZE), bf),
            pltpu.VMEM((KEY_VALUE_HEADS, HEAD_SIZE + 8, spread), f32),
            pltpu.VMEM((KEY_VALUE_HEADS, 8, spread), f32),
            pltpu.VMEM((devices, 8, spread), f32),
            pltpu.VMEM((blocks, rows, rows), f32),
            pltpu.VMEM((far, 2 * HEAD_SIZE), bf),
            pltpu.VMEM((HEAD_SIZE + SUMS, far), bf),
            pltpu.VMEM((far, UNITS * rows), f32),
            pltpu.VMEM((far, UNITS * rows), f32),
            pltpu.VMEM((8, UNITS * rows), f32),
            pltpu.VMEM((8, UNITS * rows), f32),
            pltpu.VMEM((max(1, len(late_peers(devices))) * rows, spread), bf),
            pltpu.VMEM((8, spread), f32),
            pltpu.VMEM((tokens, width), bf),
            dma((1,)),
            dma((4,)),
            dma((2,)),
            dma((blocks,)),
            dma((5,)),
            dma((devices - 1,)),
            dma((3,)),
            dma((len(stage_list(devices)) + (1 if late_peers(devices) else 0), KEY_VALUE_HEADS)),
        ],
        compiler_params=pltpu.CompilerParams(
            collective_id=0, has_side_effects=True, vmem_limit_bytes=42 * 1024 * 1024 + devices * kv_width * rows * 4
        ),
    )(
        pinned(block_lists[0]),
        pinned(list_counts[0]),
        pinned(image_blocks[0]),
        reg_owner,
        pinned(queries[0]),
        pinned(keys.reshape(blocks, rows, kv_width)),
        pinned(values.reshape(blocks, rows, kv_width)),
    )
    return out[None]


def solution(mesh):
    placed = (
        P("samp", "seq", None),
        P("samp", "seq", None),
        P("samp", "seq", None),
        P("samp"),
        P("samp", "seq", None),
        P("samp", "seq"),
        P("samp", "seq"),
    )
    return jax.shard_map(
        per_device, mesh=mesh, in_specs=placed, out_specs=P("samp", "seq", None), check_vma=False
    )
```
